256 devices in a mesh: sims: 2 (over z), rows: 16 (over y, core), fields: 8 (over x).
Axes of the slice: x: 8, y: 8, z: 2, core: 2. Of those that a mesh axis runs over, the one named last changes fastest.
The devices are a block of a 8x8x16 slice.
Arguments:
- sky_maps: float32 [6, 256, 16384], P('sims', 'rows', 'fields'), parts along dimension 0, may hold values from -7 to 7
- band_cuts: int32 [6], replicated, may hold values from 1 to 8191, as said below
- filters: float32 [3, 256, 16384], P(None, ('rows', 'fields')), may hold values from 0.3 to 3
- wiener: float32 [2, 256, 16384], P(None, ('rows', 'fields')), may hold values from 0.3 to 3
- response: float32 [256, 16384], P(('rows', 'fields')), may hold values from 0.5 to 2
Outputs:
- phi_curl: float32 [4, 256, 16384], P('sims', 'rows', 'fields'), parts along dimension 0
The draws below stay inside these ranges and needn't reach their ends.
There are 2 independent parts, one for each index of `sims`. The reference program is written for one: setup_inputs(seed, part) draws one part's arguments, and reference() takes and returns one part's arrays. A program takes and returns all parts, laid end to end along the dimension named above; an argument that names none is the same for every part. Nothing has to cross between parts.
Inputs may be any that keep to these rules, and one draw needn't show every extreme that they name: `band_cuts`: entries 0, 2 and 4 are the smallest multipole indices of the temperature, polarization and estimate bands and lie below 512; entries 1, 3 and 5 are the largest and are at least 4096.
All inputs are finite; a program needn't handle non-finite values.
Results may differ from the reference program's by a relative error of at most 0.00019.
Values sent between devices are 32-bit elements; how exact they have to be, the bound alone decides.
A program may use at most 128 MiB of HBM per device.

```python
import math
import jax
import jax.numpy as jnp

NC = 16384
NR = 256


def draw_sky_maps(key, part):
    rough_part = jax.random.normal(key, (3, NR, NC), jnp.float32)
    return jnp.clip(rough_part, -7.0, 7.0)


def draw_band_cuts(key, part):
    low_key = jax.random.fold_in(key, 3)
    high_key = jax.random.fold_in(key, 5)
    lowest = jax.random.randint(low_key, (3,), 1, max(2, NC // 32), dtype=jnp.int32)
    highest = jax.random.randint(high_key, (3,), NC // 4, NC // 2, dtype=jnp.int32)
    return jnp.stack([lowest, highest], axis=1).reshape(6)


def steps_of(own_key, shape, split, smallest, top_value):
    factor_of, own = 1.0, jax.random.fold_in(own_key, 6)
    for dim, parts in split:
        heights = jnp.exp(jax.random.uniform(jax.random.fold_in(own, dim), (parts,), jnp.float32, smallest / len(split), top_value / len(split)))
        factor_of = factor_of * jnp.repeat(heights, shape[dim] // parts).reshape([-1 if axis == dim else 1 for axis in range(len(shape))])
    return factor_of


def setup_inputs(seed: int = 0, part: int = 0) -> dict:
    keys = jax.random.split(jax.random.key(seed), 6)
    own_keys = jax.random.split(jax.random.fold_in(keys[5], part), 6)
    return {
        "sky_maps": draw_sky_maps(jax.random.fold_in(jax.random.fold_in(keys[5], part), 71), part),
        "band_cuts": draw_band_cuts(jax.random.fold_in(keys[5], 71), part),
        "filters": jnp.clip(jnp.exp(math.log(3.0) - 2.3025851 * jax.random.uniform(keys[2], (3, NR, NC), jnp.float32) ** steps_of(keys[2], (3, NR, NC), ((1, 128),), -0.2, 0.2)), 0.3, 3.0),
        "wiener": jnp.clip(jnp.exp(math.log(3.0) - 2.3025851 * jax.random.uniform(keys[3], (2, NR, NC), jnp.float32) ** steps_of(keys[3], (2, NR, NC), ((1, 128),), -0.2, 0.2)), 0.3, 3.0),
        "response": jnp.clip(jnp.exp(math.log(2.0) - 1.3862944 * jax.random.uniform(keys[4], (NR, NC), jnp.float32) ** steps_of(keys[4], (NR, NC), ((0, 128),), -0.2, 0.2)), 0.5, 2.0),
    }


def signed_index(length):
    indices = jnp.arange(length, dtype=jnp.int32)
    return jnp.where(indices < length // 2, indices, indices - length)


def reference(sky_maps, band_cuts, filters, wiener, response):
    row_ratio = NC // NR
    freq_rows = signed_index(NR)[:, None]
    freq_cols = signed_index(NC)[None, :]
    scaled_rows = row_ratio * freq_rows
    radius_sq = freq_cols * freq_cols + scaled_rows * scaled_rows

    def band_mask(lower_cut, upper_cut):
        inside = (radius_sq >= lower_cut * lower_cut) & (radius_sq <= upper_cut * upper_cut)
        return inside.astype(jnp.float32)

    mask_temp = band_mask(band_cuts[0], band_cuts[1])
    mask_pol = band_mask(band_cuts[2], band_cuts[3])
    mask_out = band_mask(band_cuts[4], band_cuts[5])
    radius_floor = jnp.maximum(radius_sq, 1).astype(jnp.float32)
    cos_two = (freq_cols * freq_cols - scaled_rows * scaled_rows).astype(jnp.float32) / radius_floor
    sin_two = (2 * freq_cols * scaled_rows).astype(jnp.float32) / radius_floor
    along_x = (2 * freq_cols).astype(jnp.float32) / NC
    along_y = (2 * freq_rows).astype(jnp.float32) / NR
    spectra = jnp.fft.fft2(sky_maps)
    temp_modes = spectra[0]
    stokes_q = spectra[1]
    stokes_u = spectra[2]
    e_modes = -(cos_two * stokes_q + sin_two * stokes_u)
    b_modes = sin_two * stokes_q - cos_two * stokes_u
    temp_bar = mask_temp * filters[0] * temp_modes
    e_bar = mask_pol * filters[1] * e_modes
    b_bar = mask_pol * filters[2] * b_modes
    rotation = cos_two + 1j * sin_two
    raising = 1j * (along_x + 1j * along_y)
    lowering = 1j * (along_x - 1j * along_y)
    pol_wiener = -(wiener[1] * e_bar) * rotation
    leg_spectra = jnp.stack([
        temp_bar,
        raising * (wiener[0] * temp_bar),
        -(e_bar + 1j * b_bar) * rotation,
        raising * pol_wiener,
        lowering * pol_wiener,
    ])
    leg_maps = jnp.fft.ifft2(leg_spectra)
    current = leg_maps[0] * leg_maps[1] + 0.5 * (jnp.conj(leg_maps[2]) * leg_maps[3] + leg_maps[2] * jnp.conj(leg_maps[4]))
    estimate = jnp.fft.ifft2(mask_out * response * (lowering * jnp.fft.fft2(current)))
    return jnp.stack([jnp.real(estimate), jnp.imag(estimate)]).astype(jnp.float32)
```

```python
import functools
import math

import jax
import jax.numpy as jnp
import numpy as np
from jax import lax
from jax.experimental import pallas as pl
from jax.experimental.pallas import tpu as pltpu
from jax.sharding import PartitionSpec as P

MESH = pl.DeviceIdType.MESH
F32 = jnp.float32
BF16 = jnp.bfloat16


def halves(table):
    high = table.astype(np.float32).astype(BF16)
    low = (table - high.astype(np.float64)).astype(np.float32).astype(BF16)
    return np.stack([np.asarray(high), np.asarray(low)])


def phases(left, right, period):
    angles = 2.0 * math.pi / period * (left[:, None] * right[None, :] % period)
    return np.cos(angles), np.sin(angles)


def tables(rows, fields, local, width):
    groups = rows * fields
    total = groups * local
    length = groups * width
    cos, sin = phases(np.arange(total), np.arange(total), total)
    forward = np.stack([np.concatenate([cos, sin], 1), np.concatenate([-sin, cos], 1)])
    forward = forward.reshape(2, groups, local, 2 * total).transpose(1, 0, 2, 3)
    along_rows = halves(forward.reshape(2 * total, 2 * total))
    place = np.arange(groups)
    block = place % fields * rows + place // fields
    cos, sin = phases(np.arange(groups), block, groups)
    same = np.eye(local)
    signed = np.stack([np.stack([cos, sin]), np.stack([-sin, cos])])
    mixed = np.einsum("cdkp,ij->cikpdj", signed, same)
    across = halves(mixed.reshape(2 * total, 2 * total))
    cos, sin = phases(np.arange(width), np.arange(width), width)
    inner = np.einsum("tcq,ij->ictqj", np.stack([cos, sin]), same)
    within = halves(inner.reshape(local * width, 2 * width * local))
    cos, sin = phases(np.arange(groups), np.arange(width), length)
    twiddle = np.stack([cos, sin]).astype(np.float32)
    return along_rows, across, within, twiddle


def dot(left, right):
    return jnp.dot(left, right, preferred_element_type=F32)


def split(value):
    high = value.astype(BF16)
    return high, (value - high.astype(F32)).astype(BF16)


def table_dot(table, value):
    high, low = split(value)
    return dot(table[0], high) + dot(table[0], low) + dot(table[1], high)


def dot_table(value, table):
    high, low = split(value)
    return dot(high, table[0]) + dot(low, table[0]) + dot(high, table[1])


def kernel(
    sizes,
    cuts,
    sky_hbm,
    filters_hbm,
    wiener_hbm,
    response_hbm,
    rows_hbm,
    across_hbm,
    within_hbm,
    twiddle_hbm,
    out_hbm,
    sky,
    raw,
    fwd_rows,
    inv_rows,
    fwd_across,
    inv_across,
    fwd_within,
    inv_within,
    twiddle,
    weights,
    sent,
    held,
    result,
    send_sems,
    recv_sems,
    load_sems,
):
    n_rows, n_fields, local, width = sizes
    groups = n_rows * n_fields
    total = groups * local
    length = groups * width
    slab = total // n_rows
    lines = 2 * local
    row_me = lax.axis_index("rows")
    field_me = lax.axis_index("fields")
    me = row_me * n_fields + field_me

    def peer(step):
        return lax.rem(row_me + step // n_fields, n_rows), lax.rem(
            field_me + lax.rem(step, n_fields), n_fields
        )

    barrier = pltpu.get_barrier_semaphore()

    def greet(step, carry):
        row, field = peer(step)
        pl.semaphore_signal(
            barrier, inc=1, device_id={"rows": row, "fields": field}, device_id_type=MESH
        )
        return carry

    lax.fori_loop(1, groups, greet, 0)

    loads = [
        pltpu.make_async_copy(source, target, load_sems.at[i])
        for i, (source, target) in enumerate(
            [
                (rows_hbm, fwd_rows),
                (across_hbm, fwd_across),
                (within_hbm, fwd_within),
                (twiddle_hbm, twiddle),
                (filters_hbm, raw.at[0:3]),
                (wiener_hbm, raw.at[3:5]),
                (response_hbm, raw.at[5:6]),
            ]
        )
    ]
    for load in loads:
        load.start()
    pl.semaphore_wait(barrier, groups - 1)

    for i in range(3):

        def scatter(step, carry, i=i):
            row = lax.rem(row_me + step, n_rows)
            pltpu.make_async_remote_copy(
                src_ref=sky_hbm.at[i, :, pl.ds(pl.multiple_of(row * width, width), width)],
                dst_ref=sky.at[i, pl.ds(row_me * slab, slab), :],
                send_sem=send_sems.at[i],
                recv_sem=recv_sems.at[i],
                device_id={"rows": row},
                device_id_type=MESH,
            ).start()
            return carry

        lax.fori_loop(1, n_rows, scatter, 0)
        pltpu.make_async_copy(
            sky_hbm.at[i, :, pl.ds(pl.multiple_of(row_me * width, width), width)],
            sky.at[i, pl.ds(row_me * slab, slab), :],
            recv_sems.at[i],
        ).start()

    def exchange(slot):
        def hand(step, carry):
            row, field = peer(step)
            pltpu.make_async_remote_copy(
                src_ref=sent.at[slot, pl.ds((row * n_fields + field) * lines, lines), :],
                dst_ref=held.at[slot, pl.ds(me * lines, lines), :],
                send_sem=send_sems.at[3 + slot],
                recv_sem=recv_sems.at[3 + slot],
                device_id={"rows": row, "fields": field},
                device_id_type=MESH,
            ).start()
            return carry

        lax.fori_loop(1, groups, hand, 0)
        pltpu.make_async_copy(
            sent.at[slot, pl.ds(me * lines, lines), :],
            held.at[slot, pl.ds(me * lines, lines), :],
            recv_sems.at[3 + slot],
        ).start()

    def arrive(slot):
        pltpu.make_async_copy(held.at[slot], held.at[slot], recv_sems.at[3 + slot]).wait()
        return held[slot]

    for load in loads:
        load.wait()
    for i in range(2):
        inv_rows[i] = fwd_rows[i].T
        inv_across[i] = fwd_across[i].T
        for t in range(2):
            span = slice(t * local * width, (t + 1) * local * width)
            inv_within[i, :, span] = fwd_within[i, :, span].T

    shape = (groups, width * local)
    k = lax.broadcasted_iota(jnp.int32, shape, 0)
    lane = lax.broadcasted_iota(jnp.int32, shape, 1)
    kx = groups * (lane // local) + k
    kx = jnp.where(kx < length // 2, kx, kx - length)
    ky = local * me + lane % local
    ky = jnp.where(ky < total // 2, ky, ky - total)
    sy = (length // total) * ky
    k2 = kx * kx + sy * sy

    def band(i):
        low, high = cuts[2 * i], cuts[2 * i + 1]
        return jnp.where((k2 >= low * low) & (k2 <= high * high), 1.0, 0.0).astype(F32)

    floor = jnp.maximum(k2, 1).astype(F32)
    cos_two = (kx * kx - sy * sy).astype(F32) / floor
    sin_two = (2 * kx * sy).astype(F32) / floor
    ux = (2 * kx).astype(F32) / length
    uy = (2 * ky).astype(F32) / total
    norm = 1.0 / (length * total)
    weights[0] = band(0) * raw[0].T * norm
    weights[1] = raw[3].T
    band_pol = band(1)
    weights[2] = band_pol * raw[1].T * norm
    weights[3] = band_pol * raw[2].T * norm
    weights[4] = raw[4].T
    out_weight = band(2) * raw[5].T * norm
    weights[5] = out_weight * uy
    weights[6] = out_weight * ux
    weights[7] = cos_two
    weights[8] = sin_two
    weights[9] = ux
    weights[10] = uy

    def sides(value):
        return jnp.concatenate([value] * local, axis=1)

    def columns_forward(value):
        mixed = table_dot(fwd_across, value)
        parts = [mixed[i * groups : (i + 1) * groups] for i in range(lines)]
        real = jnp.concatenate(parts[:local], axis=1)
        imag = jnp.concatenate(parts[local:], axis=1)
        cos, sin = sides(twiddle[0]), sides(twiddle[1])
        turned = jnp.concatenate([real * cos + imag * sin, imag * cos - real * sin], axis=0)
        out = dot_table(turned, fwd_within)
        half = width * local
        return (
            out[:groups, :half] + out[groups:, half:],
            out[groups:, :half] - out[:groups, half:],
        )

    def columns_inverse(real, imag):
        out = dot_table(jnp.concatenate([real, imag], axis=0), inv_within)
        half = width * local
        real = out[:groups, :half] - out[groups:, half:]
        imag = out[groups:, :half] + out[:groups, half:]
        cos, sin = sides(twiddle[0]), sides(twiddle[1])
        real, imag = real * cos - imag * sin, imag * cos + real * sin
        parts = [
            part[:, i * width : (i + 1) * width] for part in (real, imag) for i in range(local)
        ]
        return table_dot(inv_across, jnp.concatenate(parts, axis=0))

    for i in range(3):
        pltpu.make_async_copy(sky.at[i], sky.at[i], recv_sems.at[i]).wait()
        high, low = split(sky[i])
        sent[i] = (
            dot(fwd_rows[0, :, :total], high)
            + dot(fwd_rows[0, :, :total], low)
            + dot(fwd_rows[1, :, :total], high)
        )
        exchange(i)

    def leg(slot, real, imag):
        sent[slot] = columns_inverse(real, imag)
        exchange(slot)

    t_real, t_imag = columns_forward(arrive(0))
    t_real, t_imag = weights[0] * t_real, weights[0] * t_imag
    leg(3, t_real, t_imag)
    w_real, w_imag = weights[1] * t_real, weights[1] * t_imag
    ux, uy = weights[9], weights[10]
    leg(4, -uy * w_real - ux * w_imag, ux * w_real - uy * w_imag)
    q_real, q_imag = columns_forward(arrive(1))
    u_real, u_imag = columns_forward(arrive(2))
    cos_two, sin_two = weights[7], weights[8]
    e_real = -weights[2] * (cos_two * q_real + sin_two * u_real)
    e_imag = -weights[2] * (cos_two * q_imag + sin_two * u_imag)
    b_real = weights[3] * (sin_two * q_real - cos_two * u_real)
    b_imag = weights[3] * (sin_two * q_imag - cos_two * u_imag)
    s_real, s_imag = e_real - b_imag, e_imag + b_real
    leg(5, sin_two * s_imag - cos_two * s_real, -cos_two * s_imag - sin_two * s_real)
    w_real, w_imag = weights[4] * e_real, weights[4] * e_imag
    w_real, w_imag = sin_two * w_imag - cos_two * w_real, -cos_two * w_imag - sin_two * w_real
    leg(6, -uy * w_real - ux * w_imag, ux * w_real - uy * w_imag)
    leg(7, uy * w_real - ux * w_imag, ux * w_real + uy * w_imag)

    def to_maps(slot):
        maps = table_dot(inv_rows, arrive(slot))
        return maps[:total], maps[total:]

    a_real, a_imag = to_maps(3)
    g_real, g_imag = to_maps(4)
    c_real = a_real * g_real - a_imag * g_imag
    c_imag = a_real * g_imag + a_imag * g_real
    p_real, p_imag = to_maps(5)
    h_real, h_imag = to_maps(6)
    c_real = c_real + 0.5 * (p_real * h_real + p_imag * h_imag)
    c_imag = c_imag + 0.5 * (p_real * h_imag - p_imag * h_real)
    h_real, h_imag = to_maps(7)
    c_real = c_real + 0.5 * (p_real * h_real + p_imag * h_imag)
    c_imag = c_imag + 0.5 * (p_imag * h_real - p_real * h_imag)
    sent[8] = table_dot(fwd_rows, jnp.concatenate([c_real, c_imag], axis=0))
    exchange(8)
    c_real, c_imag = columns_forward(arrive(8))
    leg(9, weights[5] * c_real - weights[6] * c_imag, weights[6] * c_real + weights[5] * c_imag)
    e_real, e_imag = to_maps(9)
    result[0] = e_real
    result[1] = e_imag

    def gather(step, carry):
        row = lax.rem(row_me + step, n_rows)
        pltpu.make_async_remote_copy(
            src_ref=result.at[:, pl.ds(row * slab, slab), :],
            dst_ref=out_hbm.at[:, :, pl.ds(pl.multiple_of(row_me * width, width), width)],
            send_sem=send_sems.at[13],
            recv_sem=recv_sems.at[13],
            device_id={"rows": row},
            device_id_type=MESH,
        ).start()
        return carry

    lax.fori_loop(1, n_rows, gather, 0)
    pltpu.make_async_copy(
        result.at[:, pl.ds(row_me * slab, slab), :],
        out_hbm.at[:, :, pl.ds(pl.multiple_of(row_me * width, width), width)],
        recv_sems.at[13],
    ).start()
    pltpu.make_async_copy(out_hbm, out_hbm, recv_sems.at[13]).wait()
    rest = total - slab
    for i in range(3):
        block = sky.at[i, 0:rest, :]
        pltpu.make_async_copy(block, block, send_sems.at[i]).wait()
    for slot in range(10):
        block = sent.at[slot, 0 : (groups - 1) * lines, :]
        pltpu.make_async_copy(block, block, send_sems.at[3 + slot]).wait()
    block = result.at[:, 0:rest, :]
    pltpu.make_async_copy(block, block, send_sems.at[13]).wait()


def body(sizes, constants, sky_maps, band_cuts, filters, wiener, response):
    rows, fields, local, width = sizes
    groups = rows * fields
    total = groups * local

    def grid(value):
        count = value.shape[0]
        value = value.reshape(count, local, width, groups)
        return value.transpose(0, 2, 1, 3).reshape(count, width * local, groups)

    half = width * local
    anywhere = pl.BlockSpec(memory_space=pl.ANY)
    return pl.pallas_call(
        functools.partial(kernel, sizes),
        out_shape=jax.ShapeDtypeStruct((2, *sky_maps.shape[1:]), F32),
        in_specs=[pl.BlockSpec(memory_space=pltpu.SMEM)] + [anywhere] * 8,
        out_specs=anywhere,
        scratch_shapes=[
            pltpu.VMEM((3, total, width), F32),
            pltpu.VMEM((6, half, groups), F32),
            pltpu.VMEM((2, 2 * total, 2 * total), BF16),
            pltpu.VMEM((2, 2 * total, 2 * total), BF16),
            pltpu.VMEM((2, 2 * total, 2 * total), BF16),
            pltpu.VMEM((2, 2 * total, 2 * total), BF16),
            pltpu.VMEM((2, half, 2 * half), BF16),
            pltpu.VMEM((2, half, 2 * half), BF16),
            pltpu.VMEM((2, groups, width), F32),
            pltpu.VMEM((11, groups, half), F32),
            pltpu.VMEM((10, 2 * total, width), F32),
            pltpu.VMEM((10, 2 * total, width), F32),
            pltpu.VMEM((2, total, width), F32),
            pltpu.SemaphoreType.DMA((14,)),
            pltpu.SemaphoreType.DMA((14,)),
            pltpu.SemaphoreType.DMA((7,)),
        ],
        compiler_params=pltpu.CompilerParams(
            collective_id=0, has_side_effects=True, vmem_limit_bytes=40 * 1024 * 1024
        ),
    )(
        band_cuts,
        sky_maps,
        grid(filters),
        grid(wiener),
        grid(response[None]),
        *(jnp.asarray(value) for value in constants),
    )


def solution(mesh):
    placed = (
        P("sims", "rows", "fields"),
        P(),
        P(None, ("rows", "fields"), None),
        P(None, ("rows", "fields"), None),
        P(("rows", "fields"), None),
    )
    rows, fields = mesh.shape["rows"], mesh.shape["fields"]
    groups = rows * fields

    def run(sky_maps, band_cuts, filters, wiener, response):
        sizes = (rows, fields, filters.shape[1] // groups, filters.shape[2] // groups)
        constants = tables(*sizes)
        return jax.shard_map(
            functools.partial(body, sizes, constants),
            mesh=mesh,
            in_specs=placed,
            out_specs=P("sims", "rows", "fields"),
            check_vma=False,
        )(sky_maps, band_cuts, filters, wiener, response)

    return run
```

```python
import functools
import math

import jax
import jax.numpy as jnp
import numpy as np
from jax import lax
from jax.experimental import pallas as pl
from jax.experimental.pallas import tpu as pltpu
from jax.sharding import PartitionSpec as P

MESH = pl.DeviceIdType.MESH
F32 = jnp.float32
BF16 = jnp.bfloat16


def halves(table):
    high = table.astype(np.float32).astype(BF16)
    low = (table - high.astype(np.float64)).astype(np.float32).astype(BF16)
    return np.stack([np.asarray(high), np.asarray(low)])


def phases(left, right, period):
    angles = 2.0 * math.pi / period * (left[:, None] * right[None, :] % period)
    return np.cos(angles), np.sin(angles)


def tables(rows, fields, local, width):
    groups = rows * fields
    total = groups * local
    length = groups * width
    cos, sin = phases(np.arange(total), np.arange(total), total)
    forward = np.stack([np.concatenate([cos, sin], 1), np.concatenate([-sin, cos], 1)])
    forward = forward.reshape(2, groups, local, 2 * total).transpose(2, 1, 0, 3)
    forward = forward.reshape(2 * total, 2 * total)
    place = np.arange(groups)
    block = place % fields * rows + place // fields
    cos, sin = phases(np.arange(groups), block, groups)
    signed = np.stack([np.stack([cos, sin]), np.stack([-sin, cos])])
    mixed = signed.transpose(0, 2, 3, 1).reshape(2 * groups, 2 * groups)
    within = np.concatenate(phases(np.arange(width), np.arange(width), width), 1)
    cos, sin = phases(np.arange(groups), np.arange(width), length)
    twiddle = np.stack([cos, sin]).astype(np.float32)
    return (
        halves(forward),
        halves(forward.T),
        halves(mixed),
        halves(mixed.T),
        halves(within),
        twiddle,
    )


def dot(left, right):
    return jnp.dot(left, right, preferred_element_type=F32)


def split(value):
    high = value.astype(BF16)
    return high, (value - high.astype(F32)).astype(BF16)


def table_dot(table, value):
    high, low = split(value)
    return dot(table[0], high) + dot(table[0], low) + dot(table[1], high)


def dot_table(value, table):
    high, low = split(value)
    return dot(high, table[0]) + dot(low, table[0]) + dot(high, table[1])


def kernel(
    sizes,
    cuts,
    sky_hbm,
    filters_hbm,
    wiener_hbm,
    response_hbm,
    fwd_rows_hbm,
    inv_rows_hbm,
    fwd_across_hbm,
    inv_across_hbm,
    within_hbm,
    twiddle_hbm,
    out_hbm,
    sky,
    raw,
    fwd_rows,
    inv_rows,
    fwd_across,
    inv_across,
    within,
    twiddle,
    weights,
    sent,
    held,
    result,
    send_sems,
    recv_sems,
    load_sems,
):
    n_rows, n_fields, local, width = sizes
    groups = n_rows * n_fields
    total = groups * local
    length = groups * width
    slab = total // n_rows
    span = 2 * groups
    row_me = lax.axis_index("rows")
    field_me = lax.axis_index("fields")
    me = row_me * n_fields + field_me
    fields = [lax.rem(field_me + i, n_fields) for i in range(n_fields)]

    def everyone(visit):
        for field in fields[1:]:
            visit(row_me, field)

        def turn(step, carry):
            row = lax.rem(row_me + step, n_rows)
            for field in fields:
                visit(row, field)
            return carry

        lax.fori_loop(1, n_rows, turn, 0)

    barrier = pltpu.get_barrier_semaphore()

    def greet(row, field):
        pl.semaphore_signal(
            barrier, inc=1, device_id={"rows": row, "fields": field}, device_id_type=MESH
        )

    everyone(greet)

    loads = [
        pltpu.make_async_copy(source, target, load_sems.at[i])
        for i, (source, target) in enumerate(
            [
                (fwd_rows_hbm, fwd_rows),
                (filters_hbm, raw.at[0:3]),
                (wiener_hbm, raw.at[3:5]),
                (response_hbm, raw.at[5:6]),
                (fwd_across_hbm, fwd_across),
                (within_hbm, within),
                (twiddle_hbm, twiddle),
                (inv_across_hbm, inv_across),
                (inv_rows_hbm, inv_rows),
            ]
        )
    ]
    for load in loads:
        load.start()

    shape = (groups, local * width)
    k = lax.broadcasted_iota(jnp.int32, shape, 0)
    lane = lax.broadcasted_iota(jnp.int32, shape, 1)
    kx = groups * (lane % width) + k
    kx = jnp.where(kx < length // 2, kx, kx - length)
    ky = local * me + lane // width
    ky = jnp.where(ky < total // 2, ky, ky - total)
    sy = (length // total) * ky
    k2 = kx * kx + sy * sy

    def band(i):
        low, high = cuts[2 * i], cuts[2 * i + 1]
        return jnp.where((k2 >= low * low) & (k2 <= high * high), 1.0, 0.0).astype(F32)

    floor = jnp.maximum(k2, 1).astype(F32)
    weights[0] = band(0)
    weights[2] = band(1)
    weights[5] = band(2)
    weights[7] = (kx * kx - sy * sy).astype(F32) / floor
    weights[8] = (2 * kx * sy).astype(F32) / floor
    weights[9] = (2 * kx).astype(F32) / length
    weights[10] = (2 * ky).astype(F32) / total

    pl.semaphore_wait(barrier, groups - 1)

    def columns(row):
        return pl.ds(pl.multiple_of(row * width, width), width)

    for i in range(3):

        def scatter(step, carry, i=i):
            row = lax.rem(row_me + step, n_rows)
            pltpu.make_async_remote_copy(
                src_ref=sky_hbm.at[i, :, columns(row)],
                dst_ref=sky.at[i, pl.ds(row_me * slab, slab), :],
                send_sem=send_sems.at[i],
                recv_sem=recv_sems.at[i],
                device_id={"rows": row},
                device_id_type=MESH,
            ).start()
            return carry

        lax.fori_loop(1, n_rows, scatter, 0)
        pltpu.make_async_copy(
            sky_hbm.at[i, :, columns(row_me)],
            sky.at[i, pl.ds(row_me * slab, slab), :],
            recv_sems.at[i],
        ).start()

    def exchange(slot, part, sem):
        def hand(row, field):
            pltpu.make_async_remote_copy(
                src_ref=sent.at[slot, part, pl.ds((row * n_fields + field) * 2, 2), :],
                dst_ref=held.at[slot, part, pl.ds(me * 2, 2), :],
                send_sem=send_sems.at[sem],
                recv_sem=recv_sems.at[sem],
                device_id={"rows": row, "fields": field},
                device_id_type=MESH,
            ).start()

        everyone(hand)
        pltpu.make_async_copy(
            sent.at[slot, part, pl.ds(me * 2, 2), :],
            held.at[slot, part, pl.ds(me * 2, 2), :],
            recv_sems.at[sem],
        ).start()

    def arrive(slot, part, sem):
        block = held.at[slot, part]
        pltpu.make_async_copy(block, block, recv_sems.at[sem]).wait()

    both = slice(0, local)

    def sides(value, count):
        return jnp.concatenate([value] * count, axis=1)

    def stacked(real, imag):
        count = real.shape[1] // width
        return jnp.concatenate(
            [v[:, i * width : (i + 1) * width] for v in (real, imag) for i in range(count)], axis=0
        )

    def inner(real, imag, sign):
        count = real.shape[1] // width
        out = dot_table(stacked(real, imag), within)
        half = count * groups
        real = out[:half, :width] - sign * out[half:, width:]
        imag = out[half:, :width] + sign * out[:half, width:]
        parts = [
            jnp.concatenate([v[i * groups : (i + 1) * groups] for i in range(count)], axis=1)
            for v in (real, imag)
        ]
        return parts[0], parts[1]

    def columns_forward(slot, rows):
        value = jnp.concatenate([held[slot, i] for i in rows], axis=1)
        mixed = table_dot(fwd_across, value)
        real, imag = mixed[:groups], mixed[groups:]
        cos, sin = sides(twiddle[0], len(rows)), sides(twiddle[1], len(rows))
        return inner(real * cos + imag * sin, imag * cos - real * sin, -1.0)

    def columns_inverse(real, imag):
        count = real.shape[1] // width
        real, imag = inner(real, imag, 1.0)
        cos, sin = sides(twiddle[0], count), sides(twiddle[1], count)
        turned = jnp.concatenate([real * cos - imag * sin, imag * cos + real * sin], axis=0)
        return table_dot(inv_across, turned)

    loads[0].wait()
    for i in range(3):
        pltpu.make_async_copy(sky.at[i], sky.at[i], recv_sems.at[i]).wait()
        high, low = split(sky[i])
        spectra = (
            dot(fwd_rows[0, :, :total], high)
            + dot(fwd_rows[0, :, :total], low)
            + dot(fwd_rows[1, :, :total], high)
        )
        for j in range(local):
            sent[i, j] = spectra[j * span : (j + 1) * span]
        exchange(i, both, 3 + i)

    for load in loads[1:]:
        load.wait()

    def grid(i):
        rows = [raw[i, pl.ds(j, width, stride=local), :].T for j in range(local)]
        return jnp.concatenate(rows, axis=1)

    norm = 1.0 / (length * total)
    weights[0] = weights[0] * grid(0) * norm
    weights[1] = grid(3)
    band_pol = weights[2] * norm
    weights[2] = band_pol * grid(1)
    weights[3] = band_pol * grid(2)
    weights[4] = grid(4)
    out_weight = weights[5] * grid(5) * norm
    weights[5] = out_weight * weights[10]
    weights[6] = out_weight * weights[9]

    def leg(slot, real, imag):
        out = columns_inverse(real, imag)
        for j in range(local):
            sent[slot, j] = out[:, j * width : (j + 1) * width]
        exchange(slot, both, 3 + slot)

    all_rows = list(range(local))
    arrive(0, both, 3)
    t_real, t_imag = columns_forward(0, all_rows)
    t_real, t_imag = weights[0] * t_real, weights[0] * t_imag
    leg(3, t_real, t_imag)
    w_real, w_imag = weights[1] * t_real, weights[1] * t_imag
    ux, uy = weights[9], weights[10]
    leg(4, -uy * w_real - ux * w_imag, ux * w_real - uy * w_imag)
    arrive(1, both, 4)
    q_real, q_imag = columns_forward(1, all_rows)
    arrive(2, both, 5)
    u_real, u_imag = columns_forward(2, all_rows)
    cos_two, sin_two = weights[7], weights[8]
    e_real = -weights[2] * (cos_two * q_real + sin_two * u_real)
    e_imag = -weights[2] * (cos_two * q_imag + sin_two * u_imag)
    b_real = weights[3] * (sin_two * q_real - cos_two * u_real)
    b_imag = weights[3] * (sin_two * q_imag - cos_two * u_imag)
    s_real, s_imag = e_real - b_imag, e_imag + b_real
    leg(5, sin_two * s_imag - cos_two * s_real, -cos_two * s_imag - sin_two * s_real)
    w_real, w_imag = weights[4] * e_real, weights[4] * e_imag
    w_real, w_imag = sin_two * w_imag - cos_two * w_real, -cos_two * w_imag - sin_two * w_real
    leg(6, -uy * w_real - ux * w_imag, ux * w_real - uy * w_imag)
    leg(7, uy * w_real - ux * w_imag, ux * w_real + uy * w_imag)

    def to_maps(slot):
        arrive(slot, both, 3 + slot)
        value = jnp.concatenate([held[slot, j] for j in range(local)], axis=0)
        maps = table_dot(inv_rows, value)
        return maps[:total], maps[total:]

    a_real, a_imag = to_maps(3)
    g_real, g_imag = to_maps(4)
    c_real = a_real * g_real - a_imag * g_imag
    c_imag = a_real * g_imag + a_imag * g_real
    p_real, p_imag = to_maps(5)
    h_real, h_imag = to_maps(6)
    c_real = c_real + 0.5 * (p_real * h_real + p_imag * h_imag)
    c_imag = c_imag + 0.5 * (p_real * h_imag - p_imag * h_real)
    h_real, h_imag = to_maps(7)
    c_real = c_real + 0.5 * (p_real * h_real + p_imag * h_imag)
    c_imag = c_imag + 0.5 * (p_imag * h_real - p_real * h_imag)
    current = jnp.concatenate([c_real, c_imag], axis=0)
    high, low = split(current)
    for j in range(local):
        part = slice(j * span, (j + 1) * span)
        sent[8, j] = (
            dot(fwd_rows[0, part], high)
            + dot(fwd_rows[0, part], low)
            + dot(fwd_rows[1, part], high)
        )
        exchange(8, j, 11 + j)
    for j in range(local):
        arrive(8, j, 11 + j)
        c_real, c_imag = columns_forward(8, [j])
        lanes = slice(j * width, (j + 1) * width)
        down, along = weights[5, :, lanes], weights[6, :, lanes]
        sent[9, j] = columns_inverse(down * c_real - along * c_imag, along * c_real + down * c_imag)
        exchange(9, j, 11 + local + j)
    maps = None
    for j in range(local):
        arrive(9, j, 11 + local + j)
        part = slice(j * span, (j + 1) * span)
        high, low = split(held[9, j])
        added = (
            dot(inv_rows[0, :, part], high)
            + dot(inv_rows[0, :, part], low)
            + dot(inv_rows[1, :, part], high)
        )
        maps = added if maps is None else maps + added
    last = 11 + 2 * local
    result[0] = maps[:total]
    result[1] = maps[total:]

    def gather(step, carry):
        row = lax.rem(row_me + step, n_rows)
        pltpu.make_async_remote_copy(
            src_ref=result.at[:, pl.ds(row * slab, slab), :],
            dst_ref=out_hbm.at[:, :, columns(row_me)],
            send_sem=send_sems.at[last],
            recv_sem=recv_sems.at[last],
            device_id={"rows": row},
            device_id_type=MESH,
        ).start()
        return carry

    lax.fori_loop(1, n_rows, gather, 0)
    pltpu.make_async_copy(
        result.at[:, pl.ds(row_me * slab, slab), :],
        out_hbm.at[:, :, columns(row_me)],
        recv_sems.at[last],
    ).start()
    pltpu.make_async_copy(out_hbm, out_hbm, recv_sems.at[last]).wait()
    rest = total - slab

    def gone(block, sem):
        pltpu.make_async_copy(block, block, send_sems.at[sem]).wait()

    for i in range(3):
        gone(sky.at[i, 0:rest, :], i)
    for slot in range(8):
        gone(sent.at[slot, both, 0 : span - 2, :], 3 + slot)
    for j in range(local):
        gone(sent.at[8, j, 0 : span - 2, :], 11 + j)
        gone(sent.at[9, j, 0 : span - 2, :], 11 + local + j)
    gone(result.at[:, 0:rest, :], last)


def body(sizes, constants, sky_maps, band_cuts, filters, wiener, response):
    rows, fields, local, width = sizes
    groups = rows * fields
    total = groups * local

    def grid(value):
        count = value.shape[0]
        value = value.reshape(count, local, width, groups)
        return value.transpose(0, 2, 1, 3).reshape(count, width * local, groups)

    anywhere = pl.BlockSpec(memory_space=pl.ANY)
    count = 12 + 2 * local
    return pl.pallas_call(
        functools.partial(kernel, sizes),
        out_shape=jax.ShapeDtypeStruct((2, *sky_maps.shape[1:]), F32),
        in_specs=[pl.BlockSpec(memory_space=pltpu.SMEM)] + [anywhere] * 10,
        out_specs=anywhere,
        scratch_shapes=[
            pltpu.VMEM((3, total, width), F32),
            pltpu.VMEM((6, local * width, groups), F32),
            pltpu.VMEM((2, 2 * total, 2 * total), BF16),
            pltpu.VMEM((2, 2 * total, 2 * total), BF16),
            pltpu.VMEM((2, 2 * groups, 2 * groups), BF16),
            pltpu.VMEM((2, 2 * groups, 2 * groups), BF16),
            pltpu.VMEM((2, width, 2 * width), BF16),
            pltpu.VMEM((2, groups, width), F32),
            pltpu.VMEM((11, groups, local * width), F32),
            pltpu.VMEM((10, local, 2 * groups, width), F32),
            pltpu.VMEM((10, local, 2 * groups, width), F32),
            pltpu.VMEM((2, total, width), F32),
            pltpu.SemaphoreType.DMA((count,)),
            pltpu.SemaphoreType.DMA((count,)),
            pltpu.SemaphoreType.DMA((9,)),
        ],
        compiler_params=pltpu.CompilerParams(
            collective_id=0, has_side_effects=True, vmem_limit_bytes=60 * 1024 * 1024
        ),
    )(
        band_cuts,
        sky_maps,
        grid(filters),
        grid(wiener),
        grid(response[None]),
        *(jnp.asarray(value) for value in constants),
    )


def solution(mesh):
    placed = (
        P("sims", "rows", "fields"),
        P(),
        P(None, ("rows", "fields"), None),
        P(None, ("rows", "fields"), None),
        P(("rows", "fields"), None),
    )
    rows, fields = mesh.shape["rows"], mesh.shape["fields"]
    groups = rows * fields

    def run(sky_maps, band_cuts, filters, wiener, response):
        sizes = (rows, fields, filters.shape[1] // groups, filters.shape[2] // groups)
        constants = tables(*sizes)
        return jax.shard_map(
            functools.partial(body, sizes, constants),
            mesh=mesh,
            in_specs=placed,
            out_specs=P("sims", "rows", "fields"),
            check_vma=False,
        )(sky_maps, band_cuts, filters, wiener, response)

    return run
```

```python
import functools
import math

import jax
import jax.numpy as jnp
import numpy as np
from jax import lax
from jax.experimental import pallas as pl
from jax.experimental.pallas import tpu as pltpu
from jax.sharding import PartitionSpec as P

MESH = pl.DeviceIdType.MESH
F32 = jnp.float32
BF16 = jnp.bfloat16


def halves(table):
    high = table.astype(np.float32).astype(BF16)
    low = (table - high.astype(np.float64)).astype(np.float32).astype(BF16)
    return np.stack([np.asarray(high), np.asarray(low)])


def phases(left, right, period):
    angles = 2.0 * math.pi / period * (left[:, None] * right[None, :] % period)
    return np.cos(angles), np.sin(angles)


def tables(rows, fields, local, width):
    groups = rows * fields
    total = groups * local
    length = groups * width
    cos, sin = phases(np.arange(total), np.arange(total), total)
    forward = np.stack([np.concatenate([cos, sin], 1), np.concatenate([-sin, cos], 1)])
    forward = forward.reshape(2, groups, local, 2 * total).transpose(2, 1, 0, 3)
    forward = forward.reshape(2 * total, 2 * total)
    place = np.arange(groups)
    block = place % fields * rows + place // fields
    cos, sin = phases(np.arange(groups), block, groups)
    signed = np.stack([np.stack([cos, sin]), np.stack([-sin, cos])])
    mixed = signed.transpose(0, 2, 3, 1).reshape(2 * groups, 2 * groups)
    within = np.concatenate(phases(np.arange(width), np.arange(width), width), 1)
    cos, sin = phases(np.arange(groups), np.arange(width), length)
    twiddle = np.stack([cos, sin]).astype(np.float32)
    return (
        halves(forward),
        halves(forward.T),
        halves(mixed),
        halves(mixed.T),
        halves(within),
        twiddle,
    )


def dot(left, right):
    return jnp.dot(left, right, preferred_element_type=F32)


def split(value):
    high = value.astype(BF16)
    return high, (value - high.astype(F32)).astype(BF16)


def table_dot(table, value):
    high, low = split(value)
    return dot(table[0], high) + dot(table[0], low) + dot(table[1], high)


def dot_table(value, table):
    high, low = split(value)
    return dot(high, table[0]) + dot(low, table[0]) + dot(high, table[1])


def kernel(
    sizes,
    cuts_hbm,
    sky_hbm,
    filters_hbm,
    wiener_hbm,
    response_hbm,
    fwd_rows_hbm,
    inv_rows_hbm,
    fwd_across_hbm,
    inv_across_hbm,
    within_hbm,
    twiddle_hbm,
    out,
    cuts,
    local_sky,
    sky,
    raw,
    fwd_rows,
    inv_rows,
    fwd_across,
    inv_across,
    within,
    twiddle,
    weights,
    sent,
    held,
    result,
    send_sems,
    recv_sems,
    load_sems,
):
    n_rows, n_fields, local, width = sizes
    groups = n_rows * n_fields
    total = groups * local
    length = groups * width
    slab = total // n_rows
    span = 2 * groups
    row_me = lax.axis_index("rows")
    field_me = lax.axis_index("fields")
    me = row_me * n_fields + field_me
    fields = [lax.rem(field_me + i, n_fields) for i in range(n_fields)]

    def far_row(step):
        side = 1 - 2 * (step % 2)
        return lax.rem(row_me + n_rows // 2 + side * ((step + 1) // 2), n_rows)

    def everyone(visit):
        def turn(step, carry):
            row = far_row(step)
            for field in fields:
                visit(row, field)
            return carry

        lax.fori_loop(0, n_rows - 1, turn, 0)
        for field in fields[1:]:
            visit(row_me, field)

    barrier = pltpu.get_barrier_semaphore()

    def greet(row, field):
        pl.semaphore_signal(
            barrier, inc=1, device_id={"rows": row, "fields": field}, device_id_type=MESH
        )

    everyone(greet)

    loads = [
        pltpu.make_async_copy(source, target, load_sems.at[i])
        for i, (source, target) in enumerate(
            [
                (cuts_hbm, cuts),
                (sky_hbm, local_sky),
                (fwd_rows_hbm, fwd_rows),
                (filters_hbm, raw.at[0:3]),
                (wiener_hbm, raw.at[3:5]),
                (response_hbm, raw.at[5:6]),
                (fwd_across_hbm, fwd_across),
                (within_hbm, within),
                (twiddle_hbm, twiddle),
                (inv_across_hbm, inv_across),
                (inv_rows_hbm, inv_rows),
            ]
        )
    ]
    for load in loads:
        load.start()

    loads[0].wait()
    shape = (groups, local * width)
    k = lax.broadcasted_iota(jnp.int32, shape, 0)
    lane = lax.broadcasted_iota(jnp.int32, shape, 1)
    kx = groups * (lane % width) + k
    kx = jnp.where(kx < length // 2, kx, kx - length)
    ky = local * me + lane // width
    ky = jnp.where(ky < total // 2, ky, ky - total)
    sy = (length // total) * ky
    k2 = kx * kx + sy * sy

    def band(i):
        low, high = cuts[2 * i], cuts[2 * i + 1]
        return jnp.where((k2 >= low * low) & (k2 <= high * high), 1.0, 0.0).astype(F32)

    floor = jnp.maximum(k2, 1).astype(F32)
    weights[0] = band(0)
    weights[2] = band(1)
    weights[5] = band(2)
    weights[7] = (kx * kx - sy * sy).astype(F32) / floor
    weights[8] = (2 * kx * sy).astype(F32) / floor
    weights[9] = (2 * kx).astype(F32) / length
    weights[10] = (2 * ky).astype(F32) / total

    loads[1].wait()
    pl.semaphore_wait(barrier, groups - 1)

    def columns(row):
        return pl.ds(pl.multiple_of(row * width, width), width)

    for i in range(3):

        def scatter(step, carry, i=i):
            row = far_row(step)
            pltpu.make_async_remote_copy(
                src_ref=local_sky.at[i, :, columns(row)],
                dst_ref=sky.at[i, pl.ds(row_me * slab, slab), :],
                send_sem=send_sems.at[i],
                recv_sem=recv_sems.at[i],
                device_id={"rows": row},
                device_id_type=MESH,
            ).start()
            return carry

        lax.fori_loop(0, n_rows - 1, scatter, 0)
        pltpu.make_async_copy(
            local_sky.at[i, :, columns(row_me)],
            sky.at[i, pl.ds(row_me * slab, slab), :],
            recv_sems.at[i],
        ).start()

    def exchange(slot, part, sem):
        def hand(row, field):
            pltpu.make_async_remote_copy(
                src_ref=sent.at[slot, part, pl.ds((row * n_fields + field) * 2, 2), :],
                dst_ref=held.at[slot, part, pl.ds(me * 2, 2), :],
                send_sem=send_sems.at[sem],
                recv_sem=recv_sems.at[sem],
                device_id={"rows": row, "fields": field},
                device_id_type=MESH,
            ).start()

        everyone(hand)
        pltpu.make_async_copy(
            sent.at[slot, part, pl.ds(me * 2, 2), :],
            held.at[slot, part, pl.ds(me * 2, 2), :],
            recv_sems.at[sem],
        ).start()

    def arrive(slot, part, sem):
        block = held.at[slot, part]
        pltpu.make_async_copy(block, block, recv_sems.at[sem]).wait()

    both = slice(0, local)

    def sides(value, count):
        return jnp.concatenate([value] * count, axis=1)

    def stacked(real, imag):
        count = real.shape[1] // width
        return jnp.concatenate(
            [v[:, i * width : (i + 1) * width] for v in (real, imag) for i in range(count)], axis=0
        )

    def inner(real, imag, sign):
        count = real.shape[1] // width
        out = dot_table(stacked(real, imag), within)
        half = count * groups
        real = out[:half, :width] - sign * out[half:, width:]
        imag = out[half:, :width] + sign * out[:half, width:]
        parts = [
            jnp.concatenate([v[i * groups : (i + 1) * groups] for i in range(count)], axis=1)
            for v in (real, imag)
        ]
        return parts[0], parts[1]

    def columns_forward(slot, rows):
        value = jnp.concatenate([held[slot, i] for i in rows], axis=1)
        mixed = table_dot(fwd_across, value)
        real, imag = mixed[:groups], mixed[groups:]
        cos, sin = sides(twiddle[0], len(rows)), sides(twiddle[1], len(rows))
        return inner(real * cos + imag * sin, imag * cos - real * sin, -1.0)

    def columns_inverse(real, imag):
        count = real.shape[1] // width
        real, imag = inner(real, imag, 1.0)
        cos, sin = sides(twiddle[0], count), sides(twiddle[1], count)
        turned = jnp.concatenate([real * cos - imag * sin, imag * cos + real * sin], axis=0)
        return table_dot(inv_across, turned)

    loads[2].wait()
    for i in range(3):
        pltpu.make_async_copy(sky.at[i], sky.at[i], recv_sems.at[i]).wait()
        high, low = split(sky[i])
        spectra = (
            dot(fwd_rows[0, :, :total], high)
            + dot(fwd_rows[0, :, :total], low)
            + dot(fwd_rows[1, :, :total], high)
        )
        for j in range(local):
            sent[i, j] = spectra[j * span : (j + 1) * span]
        exchange(i, both, 3 + i)

    for load in loads[3:]:
        load.wait()

    def grid(i):
        rows = [raw[i, pl.ds(j, width, stride=local), :].T for j in range(local)]
        return jnp.concatenate(rows, axis=1)

    norm = 1.0 / (length * total)
    weights[0] = weights[0] * grid(0) * norm
    weights[1] = grid(3)
    band_pol = weights[2] * norm
    weights[2] = band_pol * grid(1)
    weights[3] = band_pol * grid(2)
    weights[4] = grid(4)
    out_weight = weights[5] * grid(5) * norm
    weights[5] = out_weight * weights[10]
    weights[6] = out_weight * weights[9]

    def leg(slot, real, imag):
        out = columns_inverse(real, imag)
        for j in range(local):
            sent[slot, j] = out[:, j * width : (j + 1) * width]
        exchange(slot, both, 3 + slot)

    all_rows = list(range(local))
    arrive(0, both, 3)
    t_real, t_imag = columns_forward(0, all_rows)
    t_real, t_imag = weights[0] * t_real, weights[0] * t_imag
    leg(3, t_real, t_imag)
    w_real, w_imag = weights[1] * t_real, weights[1] * t_imag
    ux, uy = weights[9], weights[10]
    leg(4, -uy * w_real - ux * w_imag, ux * w_real - uy * w_imag)
    arrive(1, both, 4)
    q_real, q_imag = columns_forward(1, all_rows)
    arrive(2, both, 5)
    u_real, u_imag = columns_forward(2, all_rows)
    cos_two, sin_two = weights[7], weights[8]
    e_real = -weights[2] * (cos_two * q_real + sin_two * u_real)
    e_imag = -weights[2] * (cos_two * q_imag + sin_two * u_imag)
    b_real = weights[3] * (sin_two * q_real - cos_two * u_real)
    b_imag = weights[3] * (sin_two * q_imag - cos_two * u_imag)
    s_real, s_imag = e_real - b_imag, e_imag + b_real
    leg(5, sin_two * s_imag - cos_two * s_real, -cos_two * s_imag - sin_two * s_real)
    w_real, w_imag = weights[4] * e_real, weights[4] * e_imag
    w_real, w_imag = sin_two * w_imag - cos_two * w_real, -cos_two * w_imag - sin_two * w_real
    leg(6, -uy * w_real - ux * w_imag, ux * w_real - uy * w_imag)
    leg(7, uy * w_real - ux * w_imag, ux * w_real + uy * w_imag)

    def to_maps(slot):
        arrive(slot, both, 3 + slot)
        value = jnp.concatenate([held[slot, j] for j in range(local)], axis=0)
        maps = table_dot(inv_rows, value)
        return maps[:total], maps[total:]

    a_real, a_imag = to_maps(3)
    g_real, g_imag = to_maps(4)
    c_real = a_real * g_real - a_imag * g_imag
    c_imag = a_real * g_imag + a_imag * g_real
    p_real, p_imag = to_maps(5)
    h_real, h_imag = to_maps(6)
    c_real = c_real + 0.5 * (p_real * h_real + p_imag * h_imag)
    c_imag = c_imag + 0.5 * (p_real * h_imag - p_imag * h_real)
    h_real, h_imag = to_maps(7)
    c_real = c_real + 0.5 * (p_real * h_real + p_imag * h_imag)
    c_imag = c_imag + 0.5 * (p_imag * h_real - p_real * h_imag)
    current = jnp.concatenate([c_real, c_imag], axis=0)
    high, low = split(current)
    for j in range(local):
        part = slice(j * span, (j + 1) * span)
        sent[8, j] = (
            dot(fwd_rows[0, part], high)
            + dot(fwd_rows[0, part], low)
            + dot(fwd_rows[1, part], high)
        )
        exchange(8, j, 11 + j)
    for j in range(local):
        arrive(8, j, 11 + j)
        c_real, c_imag = columns_forward(8, [j])
        lanes = slice(j * width, (j + 1) * width)
        down, along = weights[5, :, lanes], weights[6, :, lanes]
        sent[9, j] = columns_inverse(down * c_real - along * c_imag, along * c_real + down * c_imag)
        exchange(9, j, 11 + local + j)
    maps = None
    for j in range(local):
        arrive(9, j, 11 + local + j)
        part = slice(j * span, (j + 1) * span)
        high, low = split(held[9, j])
        added = (
            dot(inv_rows[0, :, part], high)
            + dot(inv_rows[0, :, part], low)
            + dot(inv_rows[1, :, part], high)
        )
        maps = added if maps is None else maps + added
    last = 11 + 2 * local
    result[0] = maps[:total]
    result[1] = maps[total:]

    def gather(step, carry):
        row = far_row(step)
        pltpu.make_async_remote_copy(
            src_ref=result.at[:, pl.ds(row * slab, slab), :],
            dst_ref=out.at[:, :, columns(row_me)],
            send_sem=send_sems.at[last],
            recv_sem=recv_sems.at[last],
            device_id={"rows": row},
            device_id_type=MESH,
        ).start()
        return carry

    lax.fori_loop(0, n_rows - 1, gather, 0)
    pltpu.make_async_copy(
        result.at[:, pl.ds(row_me * slab, slab), :],
        out.at[:, :, columns(row_me)],
        recv_sems.at[last],
    ).start()
    pltpu.make_async_copy(out, out, recv_sems.at[last]).wait()
    rest = total - slab

    def gone(block, sem):
        pltpu.make_async_copy(block, block, send_sems.at[sem]).wait()

    for i in range(3):
        gone(sky.at[i, 0:rest, :], i)
    for slot in range(8):
        gone(sent.at[slot, both, 0 : span - 2, :], 3 + slot)
    for j in range(local):
        gone(sent.at[8, j, 0 : span - 2, :], 11 + j)
        gone(sent.at[9, j, 0 : span - 2, :], 11 + local + j)
    gone(result.at[:, 0:rest, :], last)


def body(sizes, constants, sky_maps, band_cuts, filters, wiener, response):
    rows, fields, local, width = sizes
    groups = rows * fields
    total = groups * local

    def grid(value):
        count = value.shape[0]
        value = value.reshape(count, local, width, groups)
        return value.transpose(0, 2, 1, 3).reshape(count, width * local, groups)

    anywhere = pl.BlockSpec(memory_space=pl.ANY)
    count = 12 + 2 * local
    return pl.pallas_call(
        functools.partial(kernel, sizes),
        out_shape=pltpu.VMEM((2, *sky_maps.shape[1:]), F32),
        in_specs=[anywhere] * 11,
        out_specs=pl.BlockSpec(memory_space=pltpu.VMEM),
        scratch_shapes=[
            pltpu.SMEM(band_cuts.shape, jnp.int32),
            pltpu.VMEM(sky_maps.shape, F32),
            pltpu.VMEM((3, total, width), F32),
            pltpu.VMEM((6, local * width, groups), F32),
            pltpu.VMEM((2, 2 * total, 2 * total), BF16),
            pltpu.VMEM((2, 2 * total, 2 * total), BF16),
            pltpu.VMEM((2, 2 * groups, 2 * groups), BF16),
            pltpu.VMEM((2, 2 * groups, 2 * groups), BF16),
            pltpu.VMEM((2, width, 2 * width), BF16),
            pltpu.VMEM((2, groups, width), F32),
            pltpu.VMEM((11, groups, local * width), F32),
            pltpu.VMEM((10, local, 2 * groups, width), F32),
            pltpu.VMEM((10, local, 2 * groups, width), F32),
            pltpu.VMEM((2, total, width), F32),
            pltpu.SemaphoreType.DMA((count,)),
            pltpu.SemaphoreType.DMA((count,)),
            pltpu.SemaphoreType.DMA((11,)),
        ],
        compiler_params=pltpu.CompilerParams(
            collective_id=0, has_side_effects=True, vmem_limit_bytes=60 * 1024 * 1024
        ),
    )(
        band_cuts,
        sky_maps,
        grid(filters),
        grid(wiener),
        grid(response[None]),
        *(jnp.asarray(value) for value in constants),
    )


def solution(mesh):
    placed = (
        P("sims", "rows", "fields"),
        P(),
        P(None, ("rows", "fields"), None),
        P(None, ("rows", "fields"), None),
        P(("rows", "fields"), None),
    )
    rows, fields = mesh.shape["rows"], mesh.shape["fields"]
    groups = rows * fields

    def run(sky_maps, band_cuts, filters, wiener, response):
        sizes = (rows, fields, filters.shape[1] // groups, filters.shape[2] // groups)
        constants = tables(*sizes)
        return jax.shard_map(
            functools.partial(body, sizes, constants),
            mesh=mesh,
            in_specs=placed,
            out_specs=P("sims", "rows", "fields"),
            check_vma=False,
        )(sky_maps, band_cuts, filters, wiener, response)

    return run
```

```python
import functools
import math

import jax
import jax.numpy as jnp
import numpy as np
from jax import lax
from jax.experimental import pallas as pl
from jax.experimental.pallas import tpu as pltpu
from jax.sharding import PartitionSpec as P

MESH = pl.DeviceIdType.MESH
F32 = jnp.float32
BF16 = jnp.bfloat16


def halves(table):
    high = table.astype(np.float32).astype(BF16)
    low = (table - high.astype(np.float64)).astype(np.float32).astype(BF16)
    return np.stack([np.asarray(high), np.asarray(low)])


def phases(left, right, period):
    angles = 2.0 * math.pi / period * (left[:, None] * right[None, :] % period)
    return np.cos(angles), np.sin(angles)


def tables(rows, fields, local, width):
    groups = rows * fields
    total = groups * local
    length = groups * width
    cos, sin = phases(np.arange(total), np.arange(total), total)
    forward = np.stack([np.concatenate([cos, sin], 1), np.concatenate([-sin, cos], 1)])
    forward = forward.reshape(2, groups, local, 2 * total).transpose(2, 1, 0, 3)
    forward = forward.reshape(2 * total, 2 * total)
    place = np.arange(groups)
    block = place % fields * rows + place // fields
    cos, sin = phases(np.arange(groups), block, groups)
    signed = np.stack([np.stack([cos, sin]), np.stack([-sin, cos])])
    mixed = signed.transpose(0, 2, 3, 1).reshape(2 * groups, 2 * groups)
    within = np.concatenate(phases(np.arange(width), np.arange(width), width), 1)
    cos, sin = phases(np.arange(groups), np.arange(width), length)
    twiddle = np.stack([cos, sin]).astype(np.float32)
    return (
        halves(forward),
        halves(forward.T),
        halves(mixed),
        halves(mixed.T),
        halves(within),
        twiddle,
    )


def dot(left, right):
    return jnp.dot(left, right, preferred_element_type=F32)


def split(value):
    high = value.astype(BF16)
    return high, (value - high.astype(F32)).astype(BF16)


def table_dot(table, value):
    high, low = split(value)
    return dot(table[0], high) + dot(table[0], low) + dot(table[1], high)


def dot_table(value, table):
    high, low = split(value)
    return dot(high, table[0]) + dot(low, table[0]) + dot(high, table[1])


def kernel(
    sizes,
    cuts_hbm,
    sky_hbm,
    filters_hbm,
    wiener_hbm,
    response_hbm,
    fwd_rows_hbm,
    inv_rows_hbm,
    fwd_across_hbm,
    inv_across_hbm,
    within_hbm,
    twiddle_hbm,
    out,
    cuts,
    local_sky,
    sky,
    raw,
    fwd_rows,
    inv_rows,
    fwd_across,
    inv_across,
    within,
    twiddle,
    weights,
    sent,
    held,
    result,
    stage,
    send_sems,
    recv_sems,
    load_sems,
):
    n_rows, n_fields, local, width = sizes
    groups = n_rows * n_fields
    total = groups * local
    length = groups * width
    slab = total // n_rows
    span = 2 * groups
    row_me = lax.axis_index("rows")
    field_me = lax.axis_index("fields")
    me = row_me * n_fields + field_me
    fields = [lax.rem(field_me + i, n_fields) for i in range(n_fields)]

    def far_row(step):
        side = 1 - 2 * (step % 2)
        return lax.rem(row_me + n_rows // 2 + side * ((step + 1) // 2), n_rows)

    def everyone(visit):
        def turn(step, carry):
            row = far_row(step)
            for field in fields:
                visit(row, field)
            return carry

        lax.fori_loop(0, n_rows - 1, turn, 0)
        for field in fields[1:]:
            visit(row_me, field)

    barrier = pltpu.get_barrier_semaphore()

    def greet(row, field):
        pl.semaphore_signal(
            barrier, inc=1, device_id={"rows": row, "fields": field}, device_id_type=MESH
        )

    everyone(greet)

    loads = [
        pltpu.make_async_copy(source, target, load_sems.at[i])
        for i, (source, target) in enumerate(
            [
                (cuts_hbm, cuts),
                (sky_hbm, local_sky),
                (fwd_rows_hbm, fwd_rows),
                (filters_hbm, raw.at[0:3]),
                (wiener_hbm, raw.at[3:5]),
                (response_hbm, raw.at[5:6]),
                (fwd_across_hbm, fwd_across),
                (within_hbm, within),
                (twiddle_hbm, twiddle),
                (inv_across_hbm, inv_across),
                (inv_rows_hbm, inv_rows),
            ]
        )
    ]
    for load in loads:
        load.start()

    loads[0].wait()
    shape = (groups, local * width)
    k = lax.broadcasted_iota(jnp.int32, shape, 0)
    lane = lax.broadcasted_iota(jnp.int32, shape, 1)
    kx = groups * (lane % width) + k
    kx = jnp.where(kx < length // 2, kx, kx - length)
    ky = local * me + lane // width
    ky = jnp.where(ky < total // 2, ky, ky - total)
    sy = (length // total) * ky
    k2 = kx * kx + sy * sy

    def band(i):
        low, high = cuts[2 * i], cuts[2 * i + 1]
        return jnp.where((k2 >= low * low) & (k2 <= high * high), 1.0, 0.0).astype(F32)

    floor = jnp.maximum(k2, 1).astype(F32)
    weights[0] = band(0)
    weights[2] = band(1)
    weights[5] = band(2)
    weights[7] = (kx * kx - sy * sy).astype(F32) / floor
    weights[8] = (2 * kx * sy).astype(F32) / floor
    weights[9] = (2 * kx).astype(F32) / length
    weights[10] = (2 * ky).astype(F32) / total

    loads[1].wait()
    pl.semaphore_wait(barrier, groups - 1)

    def columns(row):
        return pl.ds(pl.multiple_of(row * width, width), width)

    for i in range(3):

        def scatter(step, carry, i=i):
            row = far_row(step)
            pltpu.make_async_remote_copy(
                src_ref=local_sky.at[i, :, columns(row)],
                dst_ref=sky.at[i, pl.ds(row_me * slab, slab), :],
                send_sem=send_sems.at[i],
                recv_sem=recv_sems.at[i],
                device_id={"rows": row},
                device_id_type=MESH,
            ).start()
            return carry

        lax.fori_loop(0, n_rows - 1, scatter, 0)
        pltpu.make_async_copy(
            local_sky.at[i, :, columns(row_me)],
            sky.at[i, pl.ds(row_me * slab, slab), :],
            recv_sems.at[i],
        ).start()

    def exchange(slot, part, sem):
        def hand(row, field):
            pltpu.make_async_remote_copy(
                src_ref=sent.at[slot, part, pl.ds((row * n_fields + field) * 2, 2), :],
                dst_ref=held.at[slot, part, pl.ds(me * 2, 2), :],
                send_sem=send_sems.at[sem],
                recv_sem=recv_sems.at[sem],
                device_id={"rows": row, "fields": field},
                device_id_type=MESH,
            ).start()

        everyone(hand)
        pltpu.make_async_copy(
            sent.at[slot, part, pl.ds(me * 2, 2), :],
            held.at[slot, part, pl.ds(me * 2, 2), :],
            recv_sems.at[sem],
        ).start()

    def arrive(slot, part, sem):
        block = held.at[slot, part]
        pltpu.make_async_copy(block, block, recv_sems.at[sem]).wait()

    both = slice(0, local)

    def sides(value, count):
        return jnp.concatenate([value] * count, axis=1)

    def stacked(real, imag):
        count = real.shape[1] // width
        return jnp.concatenate(
            [v[:, i * width : (i + 1) * width] for v in (real, imag) for i in range(count)], axis=0
        )

    def inner(real, imag, sign):
        count = real.shape[1] // width
        out = dot_table(stacked(real, imag), within)
        half = count * groups
        real = out[:half, :width] - sign * out[half:, width:]
        imag = out[half:, :width] + sign * out[:half, width:]
        parts = [
            jnp.concatenate([v[i * groups : (i + 1) * groups] for i in range(count)], axis=1)
            for v in (real, imag)
        ]
        return parts[0], parts[1]

    def columns_forward(mixed):
        real, imag = mixed[:groups], mixed[groups:]
        cos, sin = sides(twiddle[0], local), sides(twiddle[1], local)
        return inner(real * cos + imag * sin, imag * cos - real * sin, -1.0)

    def field_forward(slot):
        value = jnp.concatenate([held[slot, j] for j in range(local)], axis=1)
        return columns_forward(table_dot(fwd_across, value))

    share = width // local

    def to_parts(value):
        return [
            jnp.concatenate(
                [
                    value[:, j * width + h * share : j * width + (h + 1) * share]
                    for j in range(local)
                ],
                axis=1,
            )
            for h in range(local)
        ]

    def from_parts(parts):
        return jnp.concatenate(
            [part[:, j * share : (j + 1) * share] for j in range(local) for part in parts], axis=1
        )

    def columns_inverse(real, imag):
        count = real.shape[1] // width
        real, imag = inner(real, imag, 1.0)
        cos, sin = sides(twiddle[0], count), sides(twiddle[1], count)
        turned = jnp.concatenate([real * cos - imag * sin, imag * cos + real * sin], axis=0)
        return table_dot(inv_across, turned)

    loads[2].wait()
    for i in range(3):
        pltpu.make_async_copy(sky.at[i], sky.at[i], recv_sems.at[i]).wait()
        high, low = split(sky[i])
        spectra = (
            dot(fwd_rows[0, :, :total], high)
            + dot(fwd_rows[0, :, :total], low)
            + dot(fwd_rows[1, :, :total], high)
        )
        for j in range(local):
            sent[i, j] = spectra[j * span : (j + 1) * span]
        exchange(i, both, 3 + i)

    for load in loads[3:]:
        load.wait()

    def grid(i):
        rows = [raw[i, pl.ds(j, width, stride=local), :].T for j in range(local)]
        return jnp.concatenate(rows, axis=1)

    norm = 1.0 / (length * total)
    weights[0] = weights[0] * grid(0) * norm
    weights[1] = grid(3)
    band_pol = weights[2] * norm
    weights[2] = band_pol * grid(1)
    weights[3] = band_pol * grid(2)
    weights[4] = grid(4)
    out_weight = weights[5] * grid(5) * norm
    weights[5] = out_weight * weights[10]
    weights[6] = out_weight * weights[9]

    def sem_of(slot, h):
        return 3 + 3 + (slot - 3) * local + h

    def leg(slot, real, imag):
        parts = to_parts(columns_inverse(real, imag))
        for h in range(local):
            sent[slot, h] = parts[h]

    def send(slots):
        for h in range(local):
            for slot in slots:
                exchange(slot, h, sem_of(slot, h))

    arrive(0, both, 3)
    t_real, t_imag = field_forward(0)
    t_real, t_imag = weights[0] * t_real, weights[0] * t_imag
    leg(3, t_real, t_imag)
    send([3])
    w_real, w_imag = weights[1] * t_real, weights[1] * t_imag
    ux, uy = weights[9], weights[10]
    leg(4, -uy * w_real - ux * w_imag, ux * w_real - uy * w_imag)
    send([4])
    arrive(1, both, 4)
    q_real, q_imag = field_forward(1)
    arrive(2, both, 5)
    u_real, u_imag = field_forward(2)
    cos_two, sin_two = weights[7], weights[8]
    e_real = -weights[2] * (cos_two * q_real + sin_two * u_real)
    e_imag = -weights[2] * (cos_two * q_imag + sin_two * u_imag)
    b_real = weights[3] * (sin_two * q_real - cos_two * u_real)
    b_imag = weights[3] * (sin_two * q_imag - cos_two * u_imag)
    s_real, s_imag = e_real - b_imag, e_imag + b_real
    leg(5, sin_two * s_imag - cos_two * s_real, -cos_two * s_imag - sin_two * s_real)
    w_real, w_imag = weights[4] * e_real, weights[4] * e_imag
    w_real, w_imag = sin_two * w_imag - cos_two * w_real, -cos_two * w_imag - sin_two * w_real
    leg(6, -ux * w_imag, ux * w_real)
    leg(7, uy * w_real, uy * w_imag)
    send([5, 6, 7])

    def to_maps(slot, h):
        arrive(slot, h, sem_of(slot, h))
        part = held[slot, h]
        value = jnp.concatenate([part[:, j * share : (j + 1) * share] for j in range(local)], axis=0)
        maps = table_dot(inv_rows, value)
        return maps[:total], maps[total:]

    products = []
    for h in range(local):
        a_real, a_imag = to_maps(3, h)
        g_real, g_imag = to_maps(4, h)
        products.append((a_real * g_real - a_imag * g_imag, a_real * g_imag + a_imag * g_real))
    for h in range(local):
        c_real, c_imag = products[h]
        p_real, p_imag = to_maps(5, h)
        x_real, x_imag = to_maps(6, h)
        c_real = c_real + (p_real * x_real + p_imag * x_imag)
        y_real, y_imag = to_maps(7, h)
        c_imag = c_imag - (p_real * y_imag - p_imag * y_real)
        spectra = table_dot(fwd_rows, jnp.concatenate([c_real, c_imag], axis=0))
        sent[8, h] = jnp.concatenate(
            [spectra[j * span : (j + 1) * span] for j in range(local)], axis=1
        )
        exchange(8, h, sem_of(8, h))
    mixed = []
    for h in range(local):
        arrive(8, h, sem_of(8, h))
        mixed.append(table_dot(fwd_across, held[8, h]))
    c_real, c_imag = columns_forward(from_parts(mixed))
    down, along = weights[5], weights[6]
    leg(9, down * c_real - along * c_imag, along * c_real + down * c_imag)
    send([9])
    last = 6 + 7 * local
    for h in range(local):
        e_real, e_imag = to_maps(9, h)
        result[h, :, :share] = e_real
        result[h, :, share : 2 * share] = e_imag

        def gather(step, carry, h=h):
            row = far_row(step)
            pltpu.make_async_remote_copy(
                src_ref=result.at[h, pl.ds(row * slab, slab), :],
                dst_ref=stage.at[h, pl.ds(row_me * slab, slab), :],
                send_sem=send_sems.at[last + h],
                recv_sem=recv_sems.at[last + h],
                device_id={"rows": row},
                device_id_type=MESH,
            ).start()
            return carry

        lax.fori_loop(0, n_rows - 1, gather, 0)
        pltpu.make_async_copy(
            result.at[h, pl.ds(row_me * slab, slab), :],
            stage.at[h, pl.ds(row_me * slab, slab), :],
            recv_sems.at[last + h],
        ).start()
    for h in range(local):
        pltpu.make_async_copy(stage.at[h], stage.at[h], recv_sems.at[last + h]).wait()
    for row in range(n_rows):
        blocks = [stage[h, row * slab : (row + 1) * slab] for h in range(local)]
        for c in range(2):
            out[c, :, row * width : (row + 1) * width] = jnp.concatenate(
                [block[:, c * share : (c + 1) * share] for block in blocks], axis=1
            )
    rest = total - slab

    def gone(block, sem):
        pltpu.make_async_copy(block, block, send_sems.at[sem]).wait()

    for i in range(3):
        gone(sky.at[i, 0:rest, :], i)
    for i in range(3):
        gone(sent.at[i, both, 0 : span - 2, :], 3 + i)
    for slot in range(3, 10):
        for h in range(local):
            gone(sent.at[slot, h, 0 : span - 2, :], sem_of(slot, h))
    for h in range(local):
        gone(result.at[h, 0:rest, :], last + h)


def body(sizes, constants, sky_maps, band_cuts, filters, wiener, response):
    rows, fields, local, width = sizes
    groups = rows * fields
    total = groups * local

    def grid(value):
        count = value.shape[0]
        value = value.reshape(count, local, width, groups)
        return value.transpose(0, 2, 1, 3).reshape(count, width * local, groups)

    anywhere = pl.BlockSpec(memory_space=pl.ANY)
    count = 6 + 8 * local
    lanes = 2 * (width // local)
    return pl.pallas_call(
        functools.partial(kernel, sizes),
        out_shape=pltpu.VMEM((2, *sky_maps.shape[1:]), F32),
        in_specs=[anywhere] * 11,
        out_specs=pl.BlockSpec(memory_space=pltpu.VMEM),
        scratch_shapes=[
            pltpu.SMEM(band_cuts.shape, jnp.int32),
            pltpu.VMEM(sky_maps.shape, F32),
            pltpu.VMEM((3, total, width), F32),
            pltpu.VMEM((6, local * width, groups), F32),
            pltpu.VMEM((2, 2 * total, 2 * total), BF16),
            pltpu.VMEM((2, 2 * total, 2 * total), BF16),
            pltpu.VMEM((2, 2 * groups, 2 * groups), BF16),
            pltpu.VMEM((2, 2 * groups, 2 * groups), BF16),
            pltpu.VMEM((2, width, 2 * width), BF16),
            pltpu.VMEM((2, groups, width), F32),
            pltpu.VMEM((11, groups, local * width), F32),
            pltpu.VMEM((10, local, 2 * groups, width), F32),
            pltpu.VMEM((10, local, 2 * groups, width), F32),
            pltpu.VMEM((local, total, lanes), F32),
            pltpu.VMEM((local, total, lanes), F32),
            pltpu.SemaphoreType.DMA((count,)),
            pltpu.SemaphoreType.DMA((count,)),
            pltpu.SemaphoreType.DMA((11,)),
        ],
        compiler_params=pltpu.CompilerParams(
            collective_id=0, has_side_effects=True, vmem_limit_bytes=60 * 1024 * 1024
        ),
    )(
        band_cuts,
        sky_maps,
        grid(filters),
        grid(wiener),
        grid(response[None]),
        *(jnp.asarray(value) for value in constants),
    )


def solution(mesh):
    placed = (
        P("sims", "rows", "fields"),
        P(),
        P(None, ("rows", "fields"), None),
        P(None, ("rows", "fields"), None),
        P(("rows", "fields"), None),
    )
    rows, fields = mesh.shape["rows"], mesh.shape["fields"]
    groups = rows * fields

    def run(sky_maps, band_cuts, filters, wiener, response):
        sizes = (rows, fields, filters.shape[1] // groups, filters.shape[2] // groups)
        constants = tables(*sizes)
        return jax.shard_map(
            functools.partial(body, sizes, constants),
            mesh=mesh,
            in_specs=placed,
            out_specs=P("sims", "rows", "fields"),
            check_vma=False,
        )(sky_maps, band_cuts, filters, wiener, response)

    return run
```

```python
import functools
import math

import jax
import jax.numpy as jnp
import numpy as np
from jax import lax
from jax.experimental import pallas as pl
from jax.experimental.pallas import tpu as pltpu
from jax.sharding import PartitionSpec as P

MESH = pl.DeviceIdType.MESH
F32 = jnp.float32
BF16 = jnp.bfloat16


def halves(table):
    high = table.astype(np.float32).astype(BF16)
    low = (table - high.astype(np.float64)).astype(np.float32).astype(BF16)
    return np.stack([np.asarray(high), np.asarray(low)])


def phases(left, right, period):
    angles = 2.0 * math.pi / period * (left[:, None] * right[None, :] % period)
    return np.cos(angles), np.sin(angles)


def tables(rows, fields, local, width):
    groups = rows * fields
    total = groups * local
    length = groups * width
    cos, sin = phases(np.arange(total), np.arange(total), total)
    forward = np.stack([np.concatenate([cos, sin], 1), np.concatenate([-sin, cos], 1)])
    forward = forward.reshape(2, groups, local, 2 * total).transpose(2, 1, 0, 3)
    forward = forward.reshape(2 * total, 2 * total)
    place = np.arange(groups)
    block = place % fields * rows + place // fields
    cos, sin = phases(np.arange(groups), block, groups)
    signed = np.stack([np.stack([cos, sin]), np.stack([-sin, cos])])
    mixed = signed.transpose(0, 2, 3, 1).reshape(2 * groups, 2 * groups)
    within = np.concatenate(phases(np.arange(width), np.arange(width), width), 1)
    cos, sin = phases(np.arange(groups), np.arange(width), length)
    twiddle = np.stack([cos, sin]).astype(np.float32)
    return (
        halves(forward),
        halves(forward.T),
        halves(mixed),
        halves(mixed.T),
        halves(within),
        twiddle,
    )


def dot(left, right):
    return jnp.dot(left, right, preferred_element_type=F32)


def split(value):
    high = value.astype(BF16)
    return high, (value - high.astype(F32)).astype(BF16)


def table_dot(table, value):
    high, low = split(value)
    return dot(table[0], high) + dot(table[0], low) + dot(table[1], high)


def dot_table(value, table):
    high, low = split(value)
    return dot(high, table[0]) + dot(low, table[0]) + dot(high, table[1])


def kernel(
    sizes,
    cuts_hbm,
    sky_hbm,
    filters_hbm,
    wiener_hbm,
    response_hbm,
    fwd_rows_hbm,
    inv_rows_hbm,
    fwd_across_hbm,
    inv_across_hbm,
    within_hbm,
    twiddle_hbm,
    out,
    cuts,
    local_sky,
    sky,
    raw,
    fwd_rows,
    inv_rows,
    fwd_across,
    inv_across,
    within,
    twiddle,
    weights,
    sent,
    held,
    result,
    stage,
    send_sems,
    recv_sems,
    load_sems,
):
    n_rows, n_fields, local, width = sizes
    groups = n_rows * n_fields
    total = groups * local
    length = groups * width
    slab = total // n_rows
    span = 2 * groups
    row_me = lax.axis_index("rows")
    field_me = lax.axis_index("fields")
    me = row_me * n_fields + field_me
    fields = [lax.rem(field_me + i, n_fields) for i in range(n_fields)]

    def far_row(step):
        side = 1 - 2 * (step % 2)
        return lax.rem(row_me + n_rows // 2 + side * ((step + 1) // 2), n_rows)

    def everyone(visit):
        def turn(step, carry):
            offset, side = carry
            row = lax.rem(row_me + offset, n_rows)
            for field in fields:
                visit(row, field)
            return n_rows - 1 + side - offset, 1 - side

        lax.fori_loop(0, n_rows - 1, turn, (jnp.int32(n_rows // 2), jnp.int32(0)))
        for field in fields[1:]:
            visit(row_me, field)

    barrier = pltpu.get_barrier_semaphore()

    def greet(row, field):
        pl.semaphore_signal(
            barrier, inc=1, device_id={"rows": row, "fields": field}, device_id_type=MESH
        )

    everyone(greet)

    loads = [
        pltpu.make_async_copy(source, target, load_sems.at[i])
        for i, (source, target) in enumerate(
            [
                (cuts_hbm, cuts),
                (sky_hbm, local_sky),
                (fwd_rows_hbm, fwd_rows),
                (filters_hbm, raw.at[0:3]),
                (wiener_hbm, raw.at[3:5]),
                (response_hbm, raw.at[5:6]),
                (fwd_across_hbm, fwd_across),
                (within_hbm, within),
                (twiddle_hbm, twiddle),
                (inv_across_hbm, inv_across),
                (inv_rows_hbm, inv_rows),
            ]
        )
    ]
    for load in loads:
        load.start()

    loads[0].wait()
    shape = (groups, local * width)
    k = lax.broadcasted_iota(jnp.int32, shape, 0)
    lane = lax.broadcasted_iota(jnp.int32, shape, 1)
    kx = groups * (lane % width) + k
    kx = jnp.where(kx < length // 2, kx, kx - length)
    ky = local * me + lane // width
    ky = jnp.where(ky < total // 2, ky, ky - total)
    sy = (length // total) * ky
    k2 = kx * kx + sy * sy

    def band(i):
        low, high = cuts[2 * i], cuts[2 * i + 1]
        return jnp.where((k2 >= low * low) & (k2 <= high * high), 1.0, 0.0).astype(F32)

    floor = jnp.maximum(k2, 1).astype(F32)
    weights[0] = band(0)
    weights[2] = band(1)
    weights[5] = band(2)
    weights[7] = (kx * kx - sy * sy).astype(F32) / floor
    weights[8] = (2 * kx * sy).astype(F32) / floor
    weights[9] = (2 * kx).astype(F32) / length
    weights[10] = (2 * ky).astype(F32) / total

    loads[1].wait()
    pl.semaphore_wait(barrier, groups - 1)

    def columns(row):
        return pl.ds(pl.multiple_of(row * width, width), width)

    for i in range(3):

        def scatter(step, carry, i=i):
            row = far_row(step)
            pltpu.make_async_remote_copy(
                src_ref=local_sky.at[i, :, columns(row)],
                dst_ref=sky.at[i, pl.ds(row_me * slab, slab), :],
                send_sem=send_sems.at[i],
                recv_sem=recv_sems.at[i],
                device_id={"rows": row},
                device_id_type=MESH,
            ).start()
            return carry

        lax.fori_loop(0, n_rows - 1, scatter, 0)
        pltpu.make_async_copy(
            local_sky.at[i, :, columns(row_me)],
            sky.at[i, pl.ds(row_me * slab, slab), :],
            recv_sems.at[i],
        ).start()

    def exchange(slot, part, sem):
        def hand(row, field):
            pltpu.make_async_remote_copy(
                src_ref=sent.at[slot, part, pl.ds((row * n_fields + field) * 2, 2), :],
                dst_ref=held.at[slot, part, pl.ds(me * 2, 2), :],
                send_sem=send_sems.at[sem],
                recv_sem=recv_sems.at[sem],
                device_id={"rows": row, "fields": field},
                device_id_type=MESH,
            ).start()

        everyone(hand)
        pltpu.make_async_copy(
            sent.at[slot, part, pl.ds(me * 2, 2), :],
            held.at[slot, part, pl.ds(me * 2, 2), :],
            recv_sems.at[sem],
        ).start()

    def arrive(slot, part, sem):
        block = held.at[slot, part]
        pltpu.make_async_copy(block, block, recv_sems.at[sem]).wait()

    both = slice(0, local)

    def sides(value, count):
        return jnp.concatenate([value] * count, axis=1)

    def stacked(real, imag):
        count = real.shape[1] // width
        return jnp.concatenate(
            [v[:, i * width : (i + 1) * width] for v in (real, imag) for i in range(count)], axis=0
        )

    def inner(real, imag, sign):
        count = real.shape[1] // width
        out = dot_table(stacked(real, imag), within)
        half = count * groups
        real = out[:half, :width] - sign * out[half:, width:]
        imag = out[half:, :width] + sign * out[:half, width:]
        parts = [
            jnp.concatenate([v[i * groups : (i + 1) * groups] for i in range(count)], axis=1)
            for v in (real, imag)
        ]
        return parts[0], parts[1]

    def columns_forward(mixed):
        real, imag = mixed[:groups], mixed[groups:]
        cos, sin = sides(twiddle[0], local), sides(twiddle[1], local)
        return inner(real * cos + imag * sin, imag * cos - real * sin, -1.0)

    def field_forward(slot):
        value = jnp.concatenate([held[slot, j] for j in range(local)], axis=1)
        return columns_forward(table_dot(fwd_across, value))

    share = width // local

    def to_parts(value):
        return [
            jnp.concatenate(
                [
                    value[:, j * width + h * share : j * width + (h + 1) * share]
                    for j in range(local)
                ],
                axis=1,
            )
            for h in range(local)
        ]

    def from_parts(parts):
        return jnp.concatenate(
            [part[:, j * share : (j + 1) * share] for j in range(local) for part in parts], axis=1
        )

    def columns_inverse(real, imag):
        count = real.shape[1] // width
        real, imag = inner(real, imag, 1.0)
        cos, sin = sides(twiddle[0], count), sides(twiddle[1], count)
        turned = jnp.concatenate([real * cos - imag * sin, imag * cos + real * sin], axis=0)
        return table_dot(inv_across, turned)

    loads[2].wait()
    for i in range(3):
        pltpu.make_async_copy(sky.at[i], sky.at[i], recv_sems.at[i]).wait()
        high, low = split(sky[i])
        spectra = (
            dot(fwd_rows[0, :, :total], high)
            + dot(fwd_rows[0, :, :total], low)
            + dot(fwd_rows[1, :, :total], high)
        )
        for j in range(local):
            sent[i, j] = spectra[j * span : (j + 1) * span]
        exchange(i, both, 3 + i)

    for load in loads[3:]:
        load.wait()

    def grid(i):
        rows = [raw[i, pl.ds(j, width, stride=local), :].T for j in range(local)]
        return jnp.concatenate(rows, axis=1)

    norm = 1.0 / (length * total)
    weights[0] = weights[0] * grid(0) * norm
    weights[1] = grid(3)
    band_pol = weights[2] * norm
    weights[2] = band_pol * grid(1)
    weights[3] = band_pol * grid(2)
    weights[4] = grid(4)
    out_weight = weights[5] * grid(5) * norm
    weights[5] = out_weight * weights[10]
    weights[6] = out_weight * weights[9]

    pair = slice(5, 7)

    def sem_of(slot, h):
        if slot < 8:
            return 8 + 2 * h + slot // 7
        return 8 + (slot - 6) * local + h

    def leg(slot, real, imag):
        parts = to_parts(columns_inverse(real, imag))
        for h in range(local):
            sent[slot, h] = parts[h]

    arrive(0, both, 3)
    t_real, t_imag = field_forward(0)
    t_real, t_imag = weights[0] * t_real, weights[0] * t_imag
    leg(3, t_real, t_imag)
    exchange(3, both, 6)
    w_real, w_imag = weights[1] * t_real, weights[1] * t_imag
    ux, uy = weights[9], weights[10]
    leg(4, -uy * w_real - ux * w_imag, ux * w_real - uy * w_imag)
    exchange(4, both, 7)
    arrive(1, both, 4)
    q_real, q_imag = field_forward(1)
    arrive(2, both, 5)
    u_real, u_imag = field_forward(2)
    cos_two, sin_two = weights[7], weights[8]
    e_real = -weights[2] * (cos_two * q_real + sin_two * u_real)
    e_imag = -weights[2] * (cos_two * q_imag + sin_two * u_imag)
    b_real = weights[3] * (sin_two * q_real - cos_two * u_real)
    b_imag = weights[3] * (sin_two * q_imag - cos_two * u_imag)
    s_real, s_imag = e_real - b_imag, e_imag + b_real
    leg(5, sin_two * s_imag - cos_two * s_real, -cos_two * s_imag - sin_two * s_real)
    w_real, w_imag = weights[4] * e_real, weights[4] * e_imag
    w_real, w_imag = sin_two * w_imag - cos_two * w_real, -cos_two * w_imag - sin_two * w_real
    leg(6, -ux * w_imag, ux * w_real)
    leg(7, uy * w_real, uy * w_imag)
    for h in range(local):
        exchange(pair, h, sem_of(5, h))
        exchange(7, h, sem_of(7, h))

    def to_maps(slot, h):
        part = held[slot, h]
        value = jnp.concatenate([part[:, j * share : (j + 1) * share] for j in range(local)], axis=0)
        maps = table_dot(inv_rows, value)
        return maps[:total], maps[total:]

    arrive(3, both, 6)
    arrive(4, both, 7)
    products = []
    for h in range(local):
        a_real, a_imag = to_maps(3, h)
        g_real, g_imag = to_maps(4, h)
        products.append((a_real * g_real - a_imag * g_imag, a_real * g_imag + a_imag * g_real))
    for h in range(local):
        c_real, c_imag = products[h]
        arrive(pair, h, sem_of(5, h))
        p_real, p_imag = to_maps(5, h)
        x_real, x_imag = to_maps(6, h)
        c_real = c_real + (p_real * x_real + p_imag * x_imag)
        arrive(7, h, sem_of(7, h))
        y_real, y_imag = to_maps(7, h)
        c_imag = c_imag - (p_real * y_imag - p_imag * y_real)
        spectra = table_dot(fwd_rows, jnp.concatenate([c_real, c_imag], axis=0))
        sent[8, h] = jnp.concatenate(
            [spectra[j * span : (j + 1) * span] for j in range(local)], axis=1
        )
        exchange(8, h, sem_of(8, h))
    mixed = []
    for h in range(local):
        arrive(8, h, sem_of(8, h))
        mixed.append(table_dot(fwd_across, held[8, h]))
    c_real, c_imag = columns_forward(from_parts(mixed))
    down, along = weights[5], weights[6]
    leg(9, down * c_real - along * c_imag, along * c_real + down * c_imag)
    for h in range(local):
        exchange(9, h, sem_of(9, h))
    last = 8 + 4 * local
    for h in range(local):
        arrive(9, h, sem_of(9, h))
        e_real, e_imag = to_maps(9, h)
        result[h, :, :share] = e_real
        result[h, :, share : 2 * share] = e_imag

        def gather(step, carry, h=h):
            row = far_row(step)
            pltpu.make_async_remote_copy(
                src_ref=result.at[h, pl.ds(row * slab, slab), :],
                dst_ref=stage.at[h, pl.ds(row_me * slab, slab), :],
                send_sem=send_sems.at[last + h],
                recv_sem=recv_sems.at[last + h],
                device_id={"rows": row},
                device_id_type=MESH,
            ).start()
            return carry

        lax.fori_loop(0, n_rows - 1, gather, 0)
        pltpu.make_async_copy(
            result.at[h, pl.ds(row_me * slab, slab), :],
            stage.at[h, pl.ds(row_me * slab, slab), :],
            recv_sems.at[last + h],
        ).start()
    for h in range(local):
        pltpu.make_async_copy(stage.at[h], stage.at[h], recv_sems.at[last + h]).wait()
    for row in range(n_rows):
        blocks = [stage[h, row * slab : (row + 1) * slab] for h in range(local)]
        for c in range(2):
            out[c, :, row * width : (row + 1) * width] = jnp.concatenate(
                [block[:, c * share : (c + 1) * share] for block in blocks], axis=1
            )
    rest = total - slab

    def gone(block, sem):
        pltpu.make_async_copy(block, block, send_sems.at[sem]).wait()

    for i in range(3):
        gone(sky.at[i, 0:rest, :], i)
    for i in range(5):
        gone(sent.at[i, both, 0 : span - 2, :], 3 + i)
    for h in range(local):
        gone(sent.at[pair, h, 0 : span - 2, :], sem_of(5, h))
        for slot in range(7, 10):
            gone(sent.at[slot, h, 0 : span - 2, :], sem_of(slot, h))
    for h in range(local):
        gone(result.at[h, 0:rest, :], last + h)


def body(sizes, constants, sky_maps, band_cuts, filters, wiener, response):
    rows, fields, local, width = sizes
    groups = rows * fields
    total = groups * local

    def grid(value):
        count = value.shape[0]
        value = value.reshape(count, local, width, groups)
        return value.transpose(0, 2, 1, 3).reshape(count, width * local, groups)

    anywhere = pl.BlockSpec(memory_space=pl.ANY)
    count = 8 + 5 * local
    lanes = 2 * (width // local)
    return pl.pallas_call(
        functools.partial(kernel, sizes),
        out_shape=pltpu.VMEM((2, *sky_maps.shape[1:]), F32),
        in_specs=[anywhere] * 11,
        out_specs=pl.BlockSpec(memory_space=pltpu.VMEM),
        scratch_shapes=[
            pltpu.SMEM(band_cuts.shape, jnp.int32),
            pltpu.VMEM(sky_maps.shape, F32),
            pltpu.VMEM((3, total, width), F32),
            pltpu.VMEM((6, local * width, groups), F32),
            pltpu.VMEM((2, 2 * total, 2 * total), BF16),
            pltpu.VMEM((2, 2 * total, 2 * total), BF16),
            pltpu.VMEM((2, 2 * groups, 2 * groups), BF16),
            pltpu.VMEM((2, 2 * groups, 2 * groups), BF16),
            pltpu.VMEM((2, width, 2 * width), BF16),
            pltpu.VMEM((2, groups, width), F32),
            pltpu.VMEM((11, groups, local * width), F32),
            pltpu.VMEM((10, local, 2 * groups, width), F32),
            pltpu.VMEM((10, local, 2 * groups, width), F32),
            pltpu.VMEM((local, total, lanes), F32),
            pltpu.VMEM((local, total, lanes), F32),
            pltpu.SemaphoreType.DMA((count,)),
            pltpu.SemaphoreType.DMA((count,)),
            pltpu.SemaphoreType.DMA((11,)),
        ],
        compiler_params=pltpu.CompilerParams(
            collective_id=0, has_side_effects=True, vmem_limit_bytes=60 * 1024 * 1024
        ),
    )(
        band_cuts,
        sky_maps,
        grid(filters),
        grid(wiener),
        grid(response[None]),
        *(jnp.asarray(value) for value in constants),
    )


def solution(mesh):
    placed = (
        P("sims", "rows", "fields"),
        P(),
        P(None, ("rows", "fields"), None),
        P(None, ("rows", "fields"), None),
        P(("rows", "fields"), None),
    )
    rows, fields = mesh.shape["rows"], mesh.shape["fields"]
    groups = rows * fields

    def run(sky_maps, band_cuts, filters, wiener, response):
        sizes = (rows, fields, filters.shape[1] // groups, filters.shape[2] // groups)
        constants = tables(*sizes)
        return jax.shard_map(
            functools.partial(body, sizes, constants),
            mesh=mesh,
            in_specs=placed,
            out_specs=P("sims", "rows", "fields"),
            check_vma=False,
        )(sky_maps, band_cuts, filters, wiener, response)

    return run
```

```python
import functools
import math

import jax
import jax.numpy as jnp
import numpy as np
from jax import lax
from jax.experimental import pallas as pl
from jax.experimental.pallas import tpu as pltpu
from jax.sharding import PartitionSpec as P

MESH = pl.DeviceIdType.MESH
F32 = jnp.float32
BF16 = jnp.bfloat16


def halves(table):
    high = table.astype(np.float32).astype(BF16)
    low = (table - high.astype(np.float64)).astype(np.float32).astype(BF16)
    return np.stack([np.asarray(high), np.asarray(low)])


def phases(left, right, period):
    angles = 2.0 * math.pi / period * (left[:, None] * right[None, :] % period)
    return np.cos(angles), np.sin(angles)


def tables(rows, fields, local, width):
    groups = rows * fields
    total = groups * local
    length = groups * width
    cos, sin = phases(np.arange(total), np.arange(total), total)
    forward = np.stack([np.concatenate([cos, sin], 1), np.concatenate([-sin, cos], 1)])
    forward = forward.reshape(2, groups, local, 2 * total).transpose(2, 1, 0, 3)
    forward = forward.reshape(2 * total, 2 * total)
    place = np.arange(groups)
    block = place % fields * rows + place // fields
    cos, sin = phases(np.arange(groups), block, groups)
    signed = np.stack([np.stack([cos, sin]), np.stack([-sin, cos])])
    mixed = signed.transpose(0, 2, 3, 1).reshape(2 * groups, 2 * groups)
    within = np.concatenate(phases(np.arange(width), np.arange(width), width), 1)
    cos, sin = phases(np.arange(groups), np.arange(width), length)
    twiddle = np.stack([cos, sin]).astype(np.float32)
    return (
        halves(forward),
        halves(forward.T),
        halves(mixed),
        halves(mixed.T),
        halves(within),
        twiddle,
    )


def dot(left, right):
    return jnp.dot(left, right, preferred_element_type=F32)


def split(value):
    high = value.astype(BF16)
    return high, (value - high.astype(F32)).astype(BF16)


def table_dot(table, value):
    high, low = split(value)
    return dot(table[0], high) + dot(table[0], low) + dot(table[1], high)


def dot_table(value, table):
    high, low = split(value)
    return dot(high, table[0]) + dot(low, table[0]) + dot(high, table[1])


def kernel(
    sizes,
    cuts_hbm,
    sky_hbm,
    filters_hbm,
    wiener_hbm,
    response_hbm,
    fwd_rows_hbm,
    inv_rows_hbm,
    fwd_across_hbm,
    inv_across_hbm,
    within_hbm,
    twiddle_hbm,
    out,
    cuts,
    local_sky,
    sky,
    raw,
    fwd_rows,
    inv_rows,
    fwd_across,
    inv_across,
    within,
    twiddle,
    weights,
    sent,
    held,
    result,
    stage,
    send_sems,
    recv_sems,
    load_sems,
):
    n_rows, n_fields, local, width = sizes
    groups = n_rows * n_fields
    total = groups * local
    length = groups * width
    slab = total // n_rows
    span = 2 * groups
    row_me = lax.axis_index("rows")
    field_me = lax.axis_index("fields")
    me = row_me * n_fields + field_me
    fields = [lax.rem(field_me + i, n_fields) for i in range(n_fields)]

    def far_row(step):
        side = 1 - 2 * (step % 2)
        return lax.rem(row_me + n_rows // 2 + side * ((step + 1) // 2), n_rows)

    def everyone(visit):
        def turn(step, carry):
            offset, side = carry
            row = lax.rem(row_me + offset, n_rows)
            for field in fields:
                visit(row, field)
            return n_rows - 1 + side - offset, 1 - side

        lax.fori_loop(0, n_rows - 1, turn, (jnp.int32(n_rows // 2), jnp.int32(0)))
        for field in fields[1:]:
            visit(row_me, field)

    barrier = pltpu.get_barrier_semaphore()

    def greet(row, field):
        pl.semaphore_signal(
            barrier, inc=1, device_id={"rows": row, "fields": field}, device_id_type=MESH
        )

    everyone(greet)

    loads = [
        pltpu.make_async_copy(source, target, load_sems.at[i])
        for i, (source, target) in enumerate(
            [
                (cuts_hbm, cuts),
                (sky_hbm, local_sky),
                (fwd_rows_hbm, fwd_rows),
                (filters_hbm, raw.at[0:3]),
                (wiener_hbm, raw.at[3:5]),
                (response_hbm, raw.at[5:6]),
                (fwd_across_hbm, fwd_across),
                (within_hbm, within),
                (twiddle_hbm, twiddle),
                (inv_across_hbm, inv_across),
                (inv_rows_hbm, inv_rows),
            ]
        )
    ]
    for load in loads:
        load.start()

    loads[0].wait()
    shape = (groups, local * width)
    k = lax.broadcasted_iota(jnp.int32, shape, 0)
    lane = lax.broadcasted_iota(jnp.int32, shape, 1)
    kx = groups * (lane % width) + k
    kx = jnp.where(kx < length // 2, kx, kx - length)
    ky = local * me + lane // width
    ky = jnp.where(ky < total // 2, ky, ky - total)
    sy = (length // total) * ky
    k2 = kx * kx + sy * sy

    def band(i):
        low, high = cuts[2 * i], cuts[2 * i + 1]
        return jnp.where((k2 >= low * low) & (k2 <= high * high), 1.0, 0.0).astype(F32)

    floor = jnp.maximum(k2, 1).astype(F32)
    weights[0] = band(0)
    weights[2] = band(1)
    weights[5] = band(2)
    weights[7] = (kx * kx - sy * sy).astype(F32) / floor
    weights[8] = (2 * kx * sy).astype(F32) / floor
    weights[9] = (2 * kx).astype(F32) / length
    weights[10] = (2 * ky).astype(F32) / total

    loads[1].wait()
    pl.semaphore_wait(barrier, groups - 1)

    def columns(row):
        return pl.ds(pl.multiple_of(row * width, width), width)

    for i in range(3):

        def scatter(step, carry, i=i):
            row = far_row(step)
            pltpu.make_async_remote_copy(
                src_ref=local_sky.at[i, :, columns(row)],
                dst_ref=sky.at[i, pl.ds(row_me * slab, slab), :],
                send_sem=send_sems.at[i],
                recv_sem=recv_sems.at[i],
                device_id={"rows": row},
                device_id_type=MESH,
            ).start()
            return carry

        lax.fori_loop(0, n_rows - 1, scatter, 0)
        pltpu.make_async_copy(
            local_sky.at[i, :, columns(row_me)],
            sky.at[i, pl.ds(row_me * slab, slab), :],
            recv_sems.at[i],
        ).start()

    def exchange(slot, part, sem):
        def hand(row, field):
            pltpu.make_async_remote_copy(
                src_ref=sent.at[slot, part, pl.ds((row * n_fields + field) * 2, 2), :],
                dst_ref=held.at[slot, part, pl.ds(me * 2, 2), :],
                send_sem=send_sems.at[sem],
                recv_sem=recv_sems.at[sem],
                device_id={"rows": row, "fields": field},
                device_id_type=MESH,
            ).start()

        everyone(hand)
        pltpu.make_async_copy(
            sent.at[slot, part, pl.ds(me * 2, 2), :],
            held.at[slot, part, pl.ds(me * 2, 2), :],
            recv_sems.at[sem],
        ).start()

    def arrive(slot, part, sem):
        block = held.at[slot, part]
        pltpu.make_async_copy(block, block, recv_sems.at[sem]).wait()

    both = slice(0, local)

    def sides(value, count):
        return jnp.concatenate([value] * count, axis=1)

    def stacked(real, imag):
        count = real.shape[1] // width
        return jnp.concatenate(
            [v[:, i * width : (i + 1) * width] for v in (real, imag) for i in range(count)], axis=0
        )

    def inner(real, imag, sign):
        count = real.shape[1] // width
        out = dot_table(stacked(real, imag), within)
        half = count * groups
        real = out[:half, :width] - sign * out[half:, width:]
        imag = out[half:, :width] + sign * out[:half, width:]
        parts = [
            jnp.concatenate([v[i * groups : (i + 1) * groups] for i in range(count)], axis=1)
            for v in (real, imag)
        ]
        return parts[0], parts[1]

    def columns_forward(mixed):
        real, imag = mixed[:groups], mixed[groups:]
        cos, sin = sides(twiddle[0], local), sides(twiddle[1], local)
        return inner(real * cos + imag * sin, imag * cos - real * sin, -1.0)

    def field_forward(slot):
        value = jnp.concatenate([held[slot, j] for j in range(local)], axis=1)
        return columns_forward(table_dot(fwd_across, value))

    share = width // local

    def to_parts(value):
        return [
            jnp.concatenate(
                [
                    value[:, j * width + h * share : j * width + (h + 1) * share]
                    for j in range(local)
                ],
                axis=1,
            )
            for h in range(local)
        ]

    def from_parts(parts):
        return jnp.concatenate(
            [part[:, j * share : (j + 1) * share] for j in range(local) for part in parts], axis=1
        )

    def columns_inverse(real, imag):
        count = real.shape[1] // width
        real, imag = inner(real, imag, 1.0)
        cos, sin = sides(twiddle[0], count), sides(twiddle[1], count)
        turned = jnp.concatenate([real * cos - imag * sin, imag * cos + real * sin], axis=0)
        return table_dot(inv_across, turned)

    loads[2].wait()
    for i in range(3):
        pltpu.make_async_copy(sky.at[i], sky.at[i], recv_sems.at[i]).wait()
        high, low = split(sky[i])
        spectra = (
            dot(fwd_rows[0, :, :total], high)
            + dot(fwd_rows[0, :, :total], low)
            + dot(fwd_rows[1, :, :total], high)
        )
        for j in range(local):
            sent[i, j] = spectra[j * span : (j + 1) * span]
        exchange(i, both, 3 + i)

    for load in loads[3:]:
        load.wait()

    def grid(i):
        rows = [raw[i, pl.ds(j, width, stride=local), :].T for j in range(local)]
        return jnp.concatenate(rows, axis=1)

    norm = 1.0 / (length * total)
    weights[0] = weights[0] * grid(0) * norm
    weights[1] = grid(3)
    band_pol = weights[2] * norm
    weights[2] = band_pol * grid(1)
    weights[3] = band_pol * grid(2)
    weights[4] = grid(4)
    out_weight = weights[5] * grid(5) * norm
    weights[5] = out_weight * weights[10]
    weights[6] = out_weight * weights[9]

    pair = slice(5, 7)

    def sem_of(slot, h):
        if slot < 8:
            return 8 + 2 * h + slot // 7
        return 8 + (slot - 6) * local + h

    def leg(slot, real, imag):
        parts = to_parts(columns_inverse(real, imag))
        for h in range(local):
            sent[slot, h] = parts[h]

    arrive(0, both, 3)
    t_real, t_imag = field_forward(0)
    t_real, t_imag = weights[0] * t_real, weights[0] * t_imag
    leg(3, t_real, t_imag)
    exchange(3, both, 6)
    w_real, w_imag = weights[1] * t_real, weights[1] * t_imag
    ux, uy = weights[9], weights[10]
    leg(4, -uy * w_real - ux * w_imag, ux * w_real - uy * w_imag)
    exchange(4, both, 7)
    arrive(1, both, 4)
    q_real, q_imag = field_forward(1)
    arrive(2, both, 5)
    u_real, u_imag = field_forward(2)
    cos_two, sin_two = weights[7], weights[8]
    e_real = -weights[2] * (cos_two * q_real + sin_two * u_real)
    e_imag = -weights[2] * (cos_two * q_imag + sin_two * u_imag)
    b_real = weights[3] * (sin_two * q_real - cos_two * u_real)
    b_imag = weights[3] * (sin_two * q_imag - cos_two * u_imag)
    s_real, s_imag = e_real - b_imag, e_imag + b_real
    leg(5, sin_two * s_imag - cos_two * s_real, -cos_two * s_imag - sin_two * s_real)
    w_real, w_imag = weights[4] * e_real, weights[4] * e_imag
    w_real, w_imag = sin_two * w_imag - cos_two * w_real, -cos_two * w_imag - sin_two * w_real
    leg(6, -ux * w_imag, ux * w_real)
    leg(7, uy * w_real, uy * w_imag)
    for h in range(local):
        exchange(pair, h, sem_of(5, h))
        exchange(7, h, sem_of(7, h))

    def to_maps(slot, h):
        part = held[slot, h]
        value = jnp.concatenate([part[:, j * share : (j + 1) * share] for j in range(local)], axis=0)
        maps = table_dot(inv_rows, value)
        return maps[:total], maps[total:]

    arrive(3, both, 6)
    arrive(4, both, 7)
    for h in range(local):
        a_real, a_imag = to_maps(3, h)
        g_real, g_imag = to_maps(4, h)
        result[h, :, :share] = a_real * g_real - a_imag * g_imag
        result[h, :, share : 2 * share] = a_real * g_imag + a_imag * g_real

    def current_part(h, carry):
        arrive(pair, h, sem_of(5, h))
        p_real, p_imag = to_maps(5, h)
        x_real, x_imag = to_maps(6, h)
        c_real = result[h, :, :share] + (p_real * x_real + p_imag * x_imag)
        arrive(7, h, sem_of(7, h))
        y_real, y_imag = to_maps(7, h)
        c_imag = result[h, :, share : 2 * share] - (p_real * y_imag - p_imag * y_real)
        spectra = table_dot(fwd_rows, jnp.concatenate([c_real, c_imag], axis=0))
        sent[8, h] = jnp.concatenate(
            [spectra[j * span : (j + 1) * span] for j in range(local)], axis=1
        )
        exchange(8, h, sem_of(8, h))
        return carry

    lax.fori_loop(0, local, current_part, 0)
    mixed = []
    for h in range(local):
        arrive(8, h, sem_of(8, h))
        mixed.append(table_dot(fwd_across, held[8, h]))
    c_real, c_imag = columns_forward(from_parts(mixed))
    down, along = weights[5], weights[6]
    leg(9, down * c_real - along * c_imag, along * c_real + down * c_imag)
    for h in range(local):
        exchange(9, h, sem_of(9, h))
    last = 8 + 4 * local
    def estimate_part(h, done):
        arrive(9, h, sem_of(9, h))
        e_real, e_imag = to_maps(9, h)
        result[h, :, :share] = e_real
        result[h, :, share : 2 * share] = e_imag

        def gather(step, carry):
            row = far_row(step)
            pltpu.make_async_remote_copy(
                src_ref=result.at[h, pl.ds(row * slab, slab), :],
                dst_ref=stage.at[h, pl.ds(row_me * slab, slab), :],
                send_sem=send_sems.at[last + h],
                recv_sem=recv_sems.at[last + h],
                device_id={"rows": row},
                device_id_type=MESH,
            ).start()
            return carry

        lax.fori_loop(0, n_rows - 1, gather, 0)
        pltpu.make_async_copy(
            result.at[h, pl.ds(row_me * slab, slab), :],
            stage.at[h, pl.ds(row_me * slab, slab), :],
            recv_sems.at[last + h],
        ).start()
        return done

    lax.fori_loop(0, local, estimate_part, 0)
    for h in range(local):
        pltpu.make_async_copy(stage.at[h], stage.at[h], recv_sems.at[last + h]).wait()
    for row in range(n_rows):
        blocks = [stage[h, row * slab : (row + 1) * slab] for h in range(local)]
        for c in range(2):
            out[c, :, row * width : (row + 1) * width] = jnp.concatenate(
                [block[:, c * share : (c + 1) * share] for block in blocks], axis=1
            )
    rest = total - slab

    def gone(block, sem):
        pltpu.make_async_copy(block, block, send_sems.at[sem]).wait()

    for i in range(3):
        gone(sky.at[i, 0:rest, :], i)
    for i in range(5):
        gone(sent.at[i, both, 0 : span - 2, :], 3 + i)
    for h in range(local):
        gone(sent.at[pair, h, 0 : span - 2, :], sem_of(5, h))
        for slot in range(7, 10):
            gone(sent.at[slot, h, 0 : span - 2, :], sem_of(slot, h))
    for h in range(local):
        gone(result.at[h, 0:rest, :], last + h)


def body(sizes, constants, sky_maps, band_cuts, filters, wiener, response):
    rows, fields, local, width = sizes
    groups = rows * fields
    total = groups * local

    def grid(value):
        count = value.shape[0]
        value = value.reshape(count, local, width, groups)
        return value.transpose(0, 2, 1, 3).reshape(count, width * local, groups)

    anywhere = pl.BlockSpec(memory_space=pl.ANY)
    count = 8 + 5 * local
    lanes = 2 * (width // local)
    return pl.pallas_call(
        functools.partial(kernel, sizes),
        out_shape=pltpu.VMEM((2, *sky_maps.shape[1:]), F32),
        in_specs=[anywhere] * 11,
        out_specs=pl.BlockSpec(memory_space=pltpu.VMEM),
        scratch_shapes=[
            pltpu.SMEM(band_cuts.shape, jnp.int32),
            pltpu.VMEM(sky_maps.shape, F32),
            pltpu.VMEM((3, total, width), F32),
            pltpu.VMEM((6, local * width, groups), F32),
            pltpu.VMEM((2, 2 * total, 2 * total), BF16),
            pltpu.VMEM((2, 2 * total, 2 * total), BF16),
            pltpu.VMEM((2, 2 * groups, 2 * groups), BF16),
            pltpu.VMEM((2, 2 * groups, 2 * groups), BF16),
            pltpu.VMEM((2, width, 2 * width), BF16),
            pltpu.VMEM((2, groups, width), F32),
            pltpu.VMEM((11, groups, local * width), F32),
            pltpu.VMEM((10, local, 2 * groups, width), F32),
            pltpu.VMEM((10, local, 2 * groups, width), F32),
            pltpu.VMEM((local, total, lanes), F32),
            pltpu.VMEM((local, total, lanes), F32),
            pltpu.SemaphoreType.DMA((count,)),
            pltpu.SemaphoreType.DMA((count,)),
            pltpu.SemaphoreType.DMA((11,)),
        ],
        compiler_params=pltpu.CompilerParams(
            collective_id=0, has_side_effects=True, vmem_limit_bytes=60 * 1024 * 1024
        ),
    )(
        band_cuts,
        sky_maps,
        grid(filters),
        grid(wiener),
        grid(response[None]),
        *(jnp.asarray(value) for value in constants),
    )


def solution(mesh):
    placed = (
        P("sims", "rows", "fields"),
        P(),
        P(None, ("rows", "fields"), None),
        P(None, ("rows", "fields"), None),
        P(("rows", "fields"), None),
    )
    rows, fields = mesh.shape["rows"], mesh.shape["fields"]
    groups = rows * fields

    def run(sky_maps, band_cuts, filters, wiener, response):
        sizes = (rows, fields, filters.shape[1] // groups, filters.shape[2] // groups)
        constants = tables(*sizes)
        return jax.shard_map(
            functools.partial(body, sizes, constants),
            mesh=mesh,
            in_specs=placed,
            out_specs=P("sims", "rows", "fields"),
            check_vma=False,
        )(sky_maps, band_cuts, filters, wiener, response)

    return run
```
